256 devices in a mesh: aux: 16 (over x, z_lo), vir: 16 (over y, z_hi, core).
Axes of the slice: x: 4, y: 4, z: 8 (z_hi: 2, z_lo: 4; z = z_hi * 4 + z_lo), core: 2. Of those that a mesh axis runs over, the one named last changes fastest.
Arguments:
- factors: bfloat16 [2048, 1024, 128], P('aux', 'vir'), may hold values from -0.125 to 0.125
- trials: float32 [1, 1024, 128], P(None, 'vir', 'aux'), may hold values from -6 to 6
- occ_energy: float32 [128], replicated, may hold values from -3 to -0.5
- vir_energy: float32 [1024], P('vir'), may hold values from 0.5 to 3
Outputs:
- trial_out: float32 [1, 1024, 128], P(None, 'vir', 'aux')
- shifts: float32 [2, 1], replicated
The draws below stay inside these ranges and needn't reach their ends.
All inputs are finite; a program needn't handle non-finite values.
Results may differ from the reference program's by a relative error of at most 0.0075.
Values may be sent and summed in bfloat16 or wider, within the bound.
A program may use at most 64 MiB of HBM per device.

```python
import jax
import jax.numpy as jnp
from jax import lax

P_SIZE = 2048
OCC = 128
VIR = 1024
NT = 1
ITERS = 2


def block_scale(rng, extent, split, smallest, top_value):
    def one(axis_at, parts):
        heights = jax.random.uniform(jax.random.fold_in(jax.random.fold_in(rng, 6), axis_at), (parts,), jnp.float32, smallest / len(split), top_value / len(split))
        return jnp.repeat(jnp.exp(heights), extent[axis_at] // parts).reshape((-1,) + (1,) * (len(extent) - axis_at - 1))

    level = one(*split[0])
    for cut in split[1:]:
        level = level * one(*cut)
    return level


def noise(stream_key, shape, spread, most, cuts=(), held_as=jnp.bfloat16):
    values = spread * jax.random.normal(stream_key, shape, jnp.float32)
    if cuts:
        values = values * block_scale(stream_key, shape, cuts, -0.22, 0.18)
    return jnp.clip(values, -most, most).astype(held_as)


def setup_inputs(seed: int = 0) -> dict:
    key_of = jax.random.split(jax.random.key(seed), 5)
    return {
        "factors": noise(key_of[0], (P_SIZE, VIR, OCC), ((P_SIZE * VIR * OCC) ** -0.25), 0.125, ((0, 16), (1, 16))),
        "trials": noise(key_of[1], (NT, VIR, OCC), 1.0, 6.0, ((1, 16), (2, 16)), jnp.float32),
        "occ_energy": jnp.clip(jax.random.uniform(key_of[2], (OCC,), jnp.float32, -3.0, -0.5), -3.0, -0.5),
        "vir_energy": jnp.clip(0.5 + 2.5 * jax.random.uniform(key_of[3], (VIR,), jnp.float32) ** block_scale(key_of[3], (VIR,), ((0, 16),), -0.2, 0.2), 0.5, 3.0),
    }


def hold_round(values):
    return lax.optimization_barrier(values.astype(jnp.bfloat16)).astype(jnp.float32)

def coupling_of(factors, rounded):
    block_size = 128 if P_SIZE % 128 == 0 else P_SIZE
    blocked = factors.reshape(P_SIZE // block_size, block_size, VIR, OCC)
    rounded_wide = rounded.astype(jnp.float32)

    def add_block(running, factor_block):
        block_wide = factor_block.astype(jnp.float32)
        density = hold_round(jnp.einsum('pai,nai->np', block_wide, rounded_wide))
        pairs = hold_round(jnp.einsum('pai,naj->npij', block_wide, rounded_wide))
        partial_value = 2.0 * jnp.einsum('pai,np->nai', block_wide, density) - jnp.einsum('paj,npij->nai', block_wide, pairs)
        return (running + partial_value, None)
    start_sum = jnp.zeros((NT, VIR, OCC), jnp.float32)
    coupling, ignored = lax.scan(add_block, start_sum, blocked)
    return coupling

def reference(factors, trials, occ_energy, vir_energy):
    energy_gap = vir_energy[:, None] - occ_energy[None, :]
    trial = trials
    shift_list = []
    for iteration in range(ITERS):
        rounded = lax.optimization_barrier(trial.astype(jnp.bfloat16))
        coupling = coupling_of(factors, rounded)
        image = energy_gap[None] * rounded.astype(jnp.float32) + coupling
        quotient = lax.optimization_barrier(jnp.sum(trial * image, axis=(1, 2))) / lax.optimization_barrier(jnp.sum(trial * trial, axis=(1, 2)))
        update = trial - (image - quotient[:, None, None] * trial) / energy_gap[None]
        mean_square = lax.optimization_barrier(jnp.mean(update * update, axis=(1, 2)))
        trial = update * lax.rsqrt(mean_square + 1e-06)[:, None, None]
        shift_list.append(quotient)
    return (trial, jnp.stack(shift_list))
```

```python
import jax
import jax.numpy as jnp
from jax import lax
from jax.experimental import pallas as pl
from jax.experimental.pallas import tpu as pltpu
from jax.sharding import Mesh
from jax.sharding import PartitionSpec as P

AUX = ("aux_0", "aux_1")
VIR_AXES = ("vir_0", "vir_1", "vir_2")
X, ZL, Y, ZH, C = AUX + VIR_AXES
MESH = pl.DeviceIdType.MESH
F32, BF16 = jnp.float32, jnp.bfloat16
COUNT = 1024 * 128


def remote(src, dst, send, recv, device):
    return pltpu.make_async_remote_copy(
        src_ref=src, dst_ref=dst, send_sem=send, recv_sem=recv, device_id=device, device_id_type=MESH
    )


def kernel(
    factors, tile_in, out,
    held, start_z, start_x, part, part_in, row_y, row_y_in, row_z, row_z_in,
    step_z, step_x, sum_y, sum_x, last_z, last_y, last_x,
    f_send, f_recv, sz_send, sz_recv, ax_send, ax_recv, rs_send, rsx_recv, rsy_recv, rsz_recv,
    dz_send, dz_recv, s_send, sy_recv, sx_recv,
):
    x, zl, y, zh, c = (lax.axis_index(name) for name in (X, ZL, Y, ZH, C))
    z = zh * 4 + zl
    v = y * 4 + zh * 2 + c
    xc = x * 2 + c
    zc = z * 2 + c

    def at_v(k):
        w = lax.rem(v + k, 16)
        return w, {ZL: lax.rem(zl + 2, 4), Y: w // 4, ZH: lax.rem(w // 2, 2), C: lax.rem(w, 2)}

    def at_zc(k):
        w = lax.rem(zc + k, 16)
        return w, {ZL: lax.rem(w // 2, 4), ZH: w // 8, C: lax.rem(w, 2)}

    def at_z(k):
        w = lax.rem(z + k, 8)
        return w, {ZL: lax.rem(w, 4), ZH: w // 4}

    def at_y(k):
        w = lax.rem(y + k, 4)
        return w, {Y: w}

    def at_x(k):
        w = lax.rem(x + k, 4)
        return w, {X: w}

    def at_xc(k):
        w = lax.rem(xc + k, 8)
        return w, {X: w // 2, C: lax.rem(w, 2)}

    peers = [at_v(k)[1] for k in range(16)] + [at_zc(k)[1] for k in range(1, 16)]
    peers += [at_y(k)[1] for k in range(1, 4)] + [at_xc(k)[1] for k in range(1, 8)]
    barrier = pltpu.get_barrier_semaphore()
    for peer in peers:
        pl.semaphore_signal(barrier, inc=1, device_id=peer, device_id_type=MESH)
    pl.semaphore_wait(barrier, len(peers))

    waiting = []

    def send(copy):
        copy.start()
        waiting.append(copy)

    for k in range(1, 16):
        send(remote(tile_in, start_z.at[zc], sz_send.at[k - 1], sz_recv.at[zc], at_zc(k)[1]))
    for k in range(16):
        w, device = at_v(k)
        send(remote(
            factors.at[pl.ds(pl.multiple_of(w * 8, 8), 8)],
            held.at[:, pl.ds(pl.multiple_of(v * 64, 64), 64), :],
            f_send.at[k], f_recv.at[v], device,
        ))
    start_z[zc] = tile_in[...]
    for k in range(1, 16):
        w = at_zc(k)[0]
        remote(tile_in, start_z.at[w], sz_send.at[0], sz_recv.at[w], {C: c}).wait_recv()

    def start_tile(at, what):
        return start_z[2 * at, what] + start_z[2 * at + 1, what]

    trial, gap = start_tile(z, 0), start_tile(z, 2)
    for what in range(2):
        for half in range(2):
            rows = [start_tile(half * 4 + k, what) for k in range(4)]
            start_x[x, y, what, half] = jnp.concatenate(rows, axis=0).astype(BF16)

    def gather(buffer, number):
        base = number * 6
        for k in range(1, 4):
            send(remote(buffer.at[x, y], buffer.at[x, y], ax_send.at[base + k - 1], ax_recv.at[number * 8 + y], at_y(k)[1]))
        for k in range(1, 4):
            w = at_y(k)[0]
            remote(buffer.at[x, w], buffer.at[x, w], ax_send.at[base], ax_recv.at[number * 8 + w], {C: c}).wait_recv()
        for k in range(1, 4):
            send(remote(buffer.at[x], buffer.at[x], ax_send.at[base + 2 + k], ax_recv.at[number * 8 + 4 + x], at_x(k)[1]))

    def gather_end(buffer, number):
        for k in range(1, 4):
            w = at_x(k)[0]
            remote(buffer.at[w], buffer.at[w], ax_send.at[number * 6], ax_recv.at[number * 8 + 4 + w], {C: c}).wait_recv()

    gather(start_x, 0)
    gather_end(start_x, 0)
    for w in range(16):
        slot = held.at[:, pl.ds(w * 64, 64), :]
        remote(slot, slot, f_send.at[0], f_recv.at[w], {C: c}).wait_recv()

    def coupling_of(wide, number):
        eye = (lax.broadcasted_iota(jnp.int32, (128, 128), 0) == lax.broadcasted_iota(jnp.int32, (128, 128), 1)).astype(F32)
        mixed = []
        for q in range(4):
            two = jnp.concatenate([held[2 * q], held[2 * q + 1]], axis=1)
            pairs = jnp.dot(wide, two, preferred_element_type=F32)
            for h in range(2):
                pair = pairs[:, h * 128 : (h + 1) * 128]
                density = jnp.sum(jnp.sum(pair * eye, axis=0, keepdims=True), axis=1, keepdims=True)
                density = density.astype(BF16).astype(F32)
                mixed.append(jnp.transpose(2.0 * density * eye - pair).astype(BF16))
        mixed = jnp.concatenate(mixed, axis=1)
        for q in range(4):
            rows = jnp.concatenate([held[p, q * 256 : (q + 1) * 256, :] for p in range(8)], axis=1)
            block = lax.dot_general(mixed, rows, (((1,), (1,)), ((), ())), preferred_element_type=F32)
            for half in range(2):
                for w in range(4):
                    part[number, w * 2 + half, q] = block[w * 32 : (w + 1) * 32, half * 128 : (half + 1) * 128].astype(BF16)
        sems = number * 18
        for k in range(1, 8):
            w, device = at_xc(k)
            send(remote(part.at[number, w], part_in.at[number, xc], rs_send.at[sems + k - 1], rsx_recv.at[number * 8 + xc], device))
        total = part[number, xc].astype(F32)
        for k in range(1, 8):
            w = at_xc(k)[0]
            remote(part.at[number, 0], part_in.at[number, w], rs_send.at[sems], rsx_recv.at[number * 8 + w], {C: c}).wait_recv()
            total += part_in[number, w].astype(F32)
        row_y[number] = total
        for k in range(1, 4):
            w, device = at_y(k)
            send(remote(row_y.at[number, w], row_y_in.at[number, y], rs_send.at[sems + 6 + k], rsy_recv.at[number * 4 + y], device))
        total = row_y[number, y]
        for k in range(1, 4):
            w = at_y(k)[0]
            remote(row_y.at[number, 0], row_y_in.at[number, w], rs_send.at[sems], rsy_recv.at[number * 4 + w], {C: c}).wait_recv()
            total += row_y_in[number, w]
        for k in range(4):
            row_z[number, k] = total[k * 8 : (k + 1) * 8]
        ends = []
        for k in range(4):
            for core in range(2):
                copy = remote(
                    row_z.at[number, k], row_z_in.at[number, z], rs_send.at[sems + 10 + k * 2 + core],
                    rsz_recv.at[number * 8 + z], {ZH: c, ZL: k, C: core},
                )
                here = jnp.logical_and(c * 4 + k == z, c == core)

                @pl.when(jnp.logical_not(here))
                def _():
                    copy.start()

                @pl.when(here)
                def _():
                    pltpu.make_async_copy(row_z.at[number, k], row_z_in.at[number, z], rsz_recv.at[number * 8 + z]).start()

                ends.append((here, copy))
        for w in range(8):
            remote(row_z.at[number, 0], row_z_in.at[number, w], rs_send.at[sems], rsz_recv.at[number * 8 + w], {C: c}).wait_recv()
        for here, copy in ends:
            @pl.when(jnp.logical_not(here))
            def _():
                copy.wait_send()
        coupling = row_z_in[number, 0]
        for w in range(1, 8):
            coupling += row_z_in[number, w]
        return coupling

    def response_of(trial, coupling):
        response = gap * trial.astype(BF16).astype(F32) + coupling
        diff = trial - response / gap
        scaled = trial / gap
        products = [trial * response, trial * trial, diff * diff, diff * scaled, scaled * scaled]
        sums = [jnp.sum(product, axis=0, keepdims=True) for product in products]
        return diff, scaled, jnp.concatenate(sums + [jnp.zeros((3, 128), F32)], axis=0)

    def scalars_of(sums):
        sums = jnp.sum(sums, axis=1, keepdims=True)
        cross_sum, self_sum, diff_sum, mixed_sum, scaled_sum = (sums[k : k + 1] for k in range(5))
        shift = cross_sum / self_sum
        length = diff_sum + 2.0 * shift * mixed_sum + shift * shift * scaled_sum
        return shift, lax.rsqrt(length / COUNT + 1e-06)

    def add_up(buffer, count):
        total = buffer[0]
        for k in range(1, count):
            total += buffer[k]
        return total

    wide = [jnp.concatenate([start_x[w, k // 2, 0, k % 2] for w in range(4)], axis=0) for k in range(8)]
    coupling = coupling_of(jnp.concatenate(wide, axis=1), 0)

    diff, scaled, sums = response_of(trial, coupling)
    step_z[z, 0] = diff
    step_z[z, 1] = sums
    for k in range(1, 8):
        send(remote(step_z.at[z], step_z.at[z], dz_send.at[k - 1], dz_recv.at[z], at_z(k)[1]))
    for k in range(1, 8):
        w = at_z(k)[0]
        remote(step_z.at[w], step_z.at[w], dz_send.at[0], dz_recv.at[w], {C: c}).wait_recv()
    for half in range(2):
        rows = [step_z[half * 4 + k, 0] for k in range(4)]
        step_x[x, y, half] = jnp.concatenate(rows, axis=0).astype(BF16)
    sums = step_z[0, 1]
    for k in range(1, 8):
        sums += step_z[k, 1]

    def spread(sums, by_y, by_x, number, between):
        base = number * 6
        by_y[y] = sums
        for k in range(1, 4):
            send(remote(by_y.at[y], by_y.at[y], s_send.at[base + k - 1], sy_recv.at[number * 4 + y], at_y(k)[1]))
        between()
        for k in range(1, 4):
            w = at_y(k)[0]
            remote(by_y.at[w], by_y.at[w], s_send.at[base], sy_recv.at[number * 4 + w], {C: c}).wait_recv()
        by_x[x] = add_up(by_y, 4)
        for k in range(1, 4):
            send(remote(by_x.at[x], by_x.at[x], s_send.at[base + 2 + k], sx_recv.at[number * 4 + x], at_x(k)[1]))
        for k in range(1, 4):
            w = at_x(k)[0]
            remote(by_x.at[w], by_x.at[w], s_send.at[base], sx_recv.at[number * 4 + w], {C: c}).wait_recv()
        return add_up(by_x, 4)

    sums = spread(sums, sum_y, sum_x, 0, lambda: gather(step_x, 1))
    gather_end(step_x, 1)
    shift, scale = scalars_of(sums)
    out[8:9, :] = jnp.broadcast_to(shift, (1, 128))
    trial = (diff + shift * scaled) * scale

    wide = []
    for k in range(8):
        moved = jnp.concatenate([step_x[w, k // 2, k % 2] for w in range(4)], axis=0).astype(F32)
        old = jnp.concatenate([start_x[w, k // 2, 1, k % 2] for w in range(4)], axis=0).astype(F32)
        wide.append(((moved + shift * old) * scale).astype(BF16))
    coupling = coupling_of(jnp.concatenate(wide, axis=1), 1)

    diff, scaled, sums = response_of(trial, coupling)
    last_z[z] = sums
    for k in range(1, 8):
        send(remote(last_z.at[z], last_z.at[z], dz_send.at[6 + k], dz_recv.at[8 + z], at_z(k)[1]))
    for k in range(1, 8):
        w = at_z(k)[0]
        remote(last_z.at[w], last_z.at[w], dz_send.at[0], dz_recv.at[8 + w], {C: c}).wait_recv()
    sums = spread(add_up(last_z, 8), last_y, last_x, 1, lambda: None)
    shift, scale = scalars_of(sums)
    out[9:10, :] = jnp.broadcast_to(shift, (1, 128))
    out[0:8, :] = (diff + shift * scaled) * scale
    for copy in waiting:
        copy.wait_send()


def local(factors, trials, occ_energy, vir_energy):
    core = lax.axis_index(C)
    row = lax.axis_index(AUX) * 8
    trial = trials[0].T
    gap = vir_energy[None, :] - lax.dynamic_slice_in_dim(occ_energy, row, 8)[:, None]
    tile = jnp.stack([trial, trial / gap, gap])
    zero = jnp.zeros_like(tile)
    tile = jnp.where(core == 0, jnp.concatenate([tile, zero], axis=2), jnp.concatenate([zero, tile], axis=2))
    vmem, dma = pltpu.VMEM, pltpu.SemaphoreType.DMA
    out = pl.pallas_call(
        kernel,
        out_shape=jax.ShapeDtypeStruct((16, 128), F32),
        in_specs=[pl.BlockSpec(memory_space=pl.ANY), pl.BlockSpec(memory_space=pltpu.VMEM)],
        out_specs=pl.BlockSpec(memory_space=pltpu.VMEM),
        scratch_shapes=[
            vmem((8, 1024, 128), BF16),
            vmem((16, 3, 8, 128), F32),
            vmem((4, 4, 2, 2, 32, 128), BF16),
            vmem((2, 8, 4, 32, 128), BF16),
            vmem((2, 8, 4, 32, 128), BF16),
            vmem((2, 4, 32, 128), F32),
            vmem((2, 4, 32, 128), F32),
            vmem((2, 4, 8, 128), F32),
            vmem((2, 8, 8, 128), F32),
            vmem((8, 2, 8, 128), F32),
            vmem((4, 4, 2, 32, 128), BF16),
            vmem((4, 8, 128), F32),
            vmem((4, 8, 128), F32),
            vmem((8, 8, 128), F32),
            vmem((4, 8, 128), F32),
            vmem((4, 8, 128), F32),
            dma((16,)), dma((16,)), dma((15,)), dma((16,)), dma((12,)), dma((16,)),
            dma((36,)), dma((16,)), dma((8,)), dma((16,)),
            dma((14,)), dma((16,)), dma((12,)), dma((8,)), dma((8,)),
        ],
        compiler_params=pltpu.CompilerParams(collective_id=0, has_side_effects=True),
    )(factors, tile)
    trial = lax.dynamic_slice_in_dim(out[0:8], core * 64, 64, 1)
    return trial.T[None], out[8:10, 0:1]


def solution(mesh):
    torus = Mesh(mesh.devices.reshape(4, 4, 4, 2, 2), AUX + VIR_AXES)
    placed = (P(AUX, VIR_AXES, None), P(None, VIR_AXES, AUX), P(), P(VIR_AXES))
    return jax.shard_map(
        local, mesh=torus, in_specs=placed, out_specs=(P(None, VIR_AXES, AUX), P()), check_vma=False
    )
```

```python
import jax
import jax.numpy as jnp
from jax import lax
from jax.experimental import pallas as pl
from jax.experimental.pallas import tpu as pltpu
from jax.sharding import Mesh
from jax.sharding import PartitionSpec as P

AUX = ("aux_0", "aux_1")
VIR_AXES = ("vir_0", "vir_1", "vir_2")
X, ZL, Y, ZH, C = AUX + VIR_AXES
MESH = pl.DeviceIdType.MESH
F32, BF16 = jnp.float32, jnp.bfloat16
COUNT = 1024 * 128


def remote(src, dst, send, recv, device):
    return pltpu.make_async_remote_copy(
        src_ref=src, dst_ref=dst, send_sem=send, recv_sem=recv, device_id=device, device_id_type=MESH
    )


def kernel(
    factors, trials, occ, vir, trial_out, shift_out,
    turn, held, swap, start_z, start_x, part, part_in, row_s, row_s_in, row_z, row_z_in,
    step_z, step_x, sum_z, sum_xy,
    f_send, f_recv, swap_send, swap_recv, az_send, az_recv, as_send, as_recv, af_send, af_recv,
    rf_send, rf_recv, rs_send, rs_recv, rz_send, rz_recv, sz_send, sz_recv, sxy_send, sxy_recv,
):
    x, zl, y, zh, c = (lax.axis_index(name) for name in (X, ZL, Y, ZH, C))
    z = zh * 4 + zl
    v = y * 4 + zh * 2 + c
    other = 1 - c
    first, second = x + c * (y - x), y + c * (x - y)

    def at_v(k):
        w = lax.rem(v + k, 16)
        return w, {ZL: lax.rem(zl + 2, 4), Y: w // 4, ZH: lax.rem(w // 2, 2), C: lax.rem(w, 2)}

    def at_z(k):
        w = lax.rem(z + k, 8)
        return w, {ZL: lax.rem(w, 4), ZH: w // 4}

    def along(axis, at, k):
        w = lax.rem(at + k, 4)
        return w, {axis: w}

    def at_first(k, core):
        w = lax.rem(first + k, 4)
        return w, {X: x + (1 - c) * (w - x), Y: y + c * (w - y), C: core}

    def at_second(k):
        w = lax.rem(second + k, 4)
        return w, {X: x + c * (w - x), Y: y + (1 - c) * (w - y)}

    def at_xy(k):
        w = lax.rem(x * 4 + y + k, 16)
        return w, {X: w // 4, Y: lax.rem(w, 4)}

    peers = [at_v(k)[1] for k in range(16)] + [at_xy(k)[1] for k in range(1, 16)] + [{C: other}]
    for k in range(1, 8):
        peers += [at_z(k)[1] | {C: core} for core in range(2)]
    for axis, at in ((X, x), (Y, y)):
        peers += [along(axis, at, k)[1] | {C: other} for k in range(1, 4)]
    barrier = pltpu.get_barrier_semaphore()
    for peer in peers:
        pl.semaphore_signal(barrier, inc=1, device_id=peer, device_id_type=MESH)

    mine = lax.broadcasted_iota(jnp.int32, (8, 128), 1) // 64 == c
    swap[0, 0:8] = jnp.where(mine, jnp.concatenate([trials[...], trials[...]], axis=1), 0.0)
    swap[0, 8:16] = jnp.where(mine, jnp.broadcast_to(jnp.concatenate([vir[...], vir[...]], axis=1), (8, 128)), 0.0)
    turn[...] = jnp.transpose(jnp.broadcast_to(occ[...], (128, 128)))
    occ_rows = turn[pl.ds(pl.multiple_of((x * 4 + zl) * 8, 8), 8), :]
    pl.semaphore_wait(barrier, len(peers))

    waiting = []

    def send(copy):
        copy.start()
        waiting.append(copy)

    def send_factors(k):
        w, device = at_v(k)
        send(remote(
            factors.at[pl.ds(pl.multiple_of(w * 8, 8), 8)],
            held.at[:, pl.ds(pl.multiple_of(v * 64, 64), 64), :],
            f_send.at[k], f_recv.at[v], device,
        ))

    def arrived(ref, sem):
        remote(ref, ref, swap_send, sem, {C: other}).wait_recv()

    swapped = remote(swap.at[0], swap.at[1], swap_send, swap_recv, {C: other})
    swapped.start()
    for k in range(4):
        send_factors(k)
    swapped.wait()
    full = swap[0] + swap[1]
    trial = full[0:8]
    gap = full[8:16] - occ_rows

    def along_z(buffer, value, number):
        base = number * 7

        @pl.when(zh == c)
        def _():
            buffer[zl] = value
            for k in range(1, 8):
                remote(buffer.at[zl], buffer.at[zl], az_send.at[base + k - 1], az_recv.at[number * 4 + zl], at_z(k)[1]).start()

    def along_z_end(buffer, number):
        for k in range(1, 4):
            w = lax.rem(zl + k, 4)
            arrived(buffer.at[w], az_recv.at[number * 4 + w])

        @pl.when(zh != c)
        def _():
            arrived(buffer.at[zl], az_recv.at[number * 4 + zl])

    def along_z_sent(buffer, number):
        base = number * 7

        @pl.when(zh == c)
        def _():
            for k in range(1, 8):
                remote(buffer.at[zl], buffer.at[zl], az_send.at[base + k - 1], az_recv.at[number * 4 + zl], at_z(k)[1]).wait_send()

    def gather(buffer, number):
        sent, got = number * 3, number * 4
        for k in range(1, 4):
            send(remote(buffer.at[c, first, second], buffer.at[c, first, second], as_send.at[sent + k - 1], as_recv.at[got + second], at_second(k)[1]))
        for k in range(1, 4):
            w = at_second(k)[0]
            arrived(buffer.at[c, first, w], as_recv.at[got + w])
        sent, got = number * 7, number * 8
        for k in range(1, 4):
            for core in range(2):
                send(remote(buffer.at[c, first], buffer.at[c, first], af_send.at[sent + k * 2 - 2 + core], af_recv.at[got + c * 4 + first], at_first(k, core)[1]))
        send(remote(buffer.at[c, first], buffer.at[c, first], af_send.at[sent + 6], af_recv.at[got + c * 4 + first], {C: other}))

    def gather_end(buffer, number):
        got = number * 8
        for half, at in ((0, x), (1, y)):
            for k in range(1, 4):
                w = lax.rem(at + k, 4)
                arrived(buffer.at[half, w], af_recv.at[got + half * 4 + w])
        far = x + y - first
        arrived(buffer.at[other, far], af_recv.at[got + other * 4 + far])

    along_z(start_z, jnp.concatenate([trial, trial / gap], axis=0).astype(BF16), 0)
    for k in range(4, 16):
        send_factors(k)
    along_z_end(start_z, 0)
    for what in range(2):
        rows = [start_z[k].astype(F32)[what * 8 : what * 8 + 8] for k in range(4)]
        start_x[c, first, second, what] = jnp.concatenate(rows, axis=0).astype(BF16)
    gather(start_x, 0)
    gather_end(start_x, 0)
    for w in range(16):
        arrived(held.at[:, pl.ds(w * 64, 64), :], f_recv.at[w])

    def coupling_of(wide, number):
        eye = (lax.broadcasted_iota(jnp.int32, (128, 128), 0) == lax.broadcasted_iota(jnp.int32, (128, 128), 1)).astype(F32)
        mixed = []
        for q in range(4):
            two = jnp.concatenate([held[2 * q], held[2 * q + 1]], axis=1)
            pairs = jnp.dot(wide, two, preferred_element_type=F32)
            for h in range(2):
                pair = pairs[:, h * 128 : (h + 1) * 128]
                density = jnp.sum(jnp.sum(pair * eye, axis=0, keepdims=True), axis=1, keepdims=True)
                density = density.astype(BF16).astype(F32)
                mixed.append(jnp.transpose(2.0 * density * eye - pair).astype(BF16))
        mixed = jnp.concatenate(mixed, axis=1)
        for q in range(4):
            rows = jnp.concatenate([held[p, q * 256 : (q + 1) * 256, :] for p in range(8)], axis=1)
            block = lax.dot_general(mixed, rows, (((1,), (1,)), ((), ())), preferred_element_type=F32).astype(BF16)
            for w in range(4):
                part[number, 0, w, q] = block[w * 32 : (w + 1) * 32, 0:128]
                part[number, 1, q, w] = block[w * 32 : (w + 1) * 32, 128:256]

        sent, got = number * 7, number * 8
        for half, axis, at in ((0, X, x), (1, Y, y)):
            for k in range(1, 4):
                w, device = along(axis, at, k)
                send(remote(
                    part.at[number, half, w], part_in.at[number, c, at], rf_send.at[sent + half * 3 + k - 1],
                    rf_recv.at[got + c * 4 + at], device | {C: half},
                ))
        far = x + y - first
        send(remote(part.at[number, other, far], part_in.at[number, c, far], rf_send.at[sent + 6], rf_recv.at[got + c * 4 + far], {C: other}))
        total = part[number, c, first].astype(F32)
        arrived(part_in.at[number, other, first], rf_recv.at[got + other * 4 + first])
        total += part_in[number, other, first].astype(F32)
        for k in range(1, 4):
            w = lax.rem(first + k, 4)
            for core in range(2):
                arrived(part_in.at[number, core, w], rf_recv.at[got + core * 4 + w])
                total += part_in[number, core, w].astype(F32)

        row_s[number] = total.astype(BF16)
        sent, got = number * 3, number * 4
        for k in range(1, 4):
            w, device = at_second(k)
            send(remote(row_s.at[number, w], row_s_in.at[number, second], rs_send.at[sent + k - 1], rs_recv.at[got + second], device))
        total = row_s[number, second].astype(F32)
        for k in range(1, 4):
            w = lax.rem(second + k, 4)
            arrived(row_s_in.at[number, w], rs_recv.at[got + w])
            total += row_s_in[number, w].astype(F32)

        for k in range(4):
            row_z[number, k] = total[k * 8 : (k + 1) * 8]
        sent, got = number * 8, number * 8
        here = zh == c
        for k in range(1, 4):
            w = lax.rem(zl + k, 4)
            for core in range(2):
                send(remote(row_z.at[number, w], row_z_in.at[number, z], rz_send.at[sent + k * 2 + core], rz_recv.at[got + z], {ZH: c, ZL: w, C: core}))
        send(remote(row_z.at[number, zl], row_z_in.at[number, z], rz_send.at[sent], rz_recv.at[got + z], {ZH: c, C: other}))
        again = remote(row_z.at[number, zl], row_z_in.at[number, z], rz_send.at[sent + 1], rz_recv.at[got + z], {ZH: c})
        local = pltpu.make_async_copy(row_z.at[number, zl], row_z_in.at[number, z], rz_recv.at[got + z])

        @pl.when(here)
        def _():
            local.start()

        @pl.when(jnp.logical_not(here))
        def _():
            again.start()

        for w in range(8):
            arrived(row_z_in.at[number, w], rz_recv.at[got + w])

        @pl.when(jnp.logical_not(here))
        def _():
            again.wait_send()

        coupling = row_z_in[number, 0]
        for w in range(1, 8):
            coupling += row_z_in[number, w]
        return coupling

    lane = lax.broadcasted_iota(jnp.int32, (1, 128), 1)

    def response_of(trial, coupling):
        response = gap * trial.astype(BF16).astype(F32) + coupling
        diff = trial - response / gap
        scaled = trial / gap
        products = [trial * response, trial * trial, diff * diff, diff * scaled, scaled * scaled]
        sums = jnp.zeros((1, 128), F32)
        for k, product in enumerate(products):
            product = jnp.sum(jnp.sum(product, axis=0, keepdims=True), axis=1, keepdims=True)
            sums = jnp.where(lane == k, product, sums)
        return diff, scaled, sums

    def sums_along_z(sums, number):
        sum_z[number, z, 0:1] = sums
        for k in range(1, 8):
            row = sum_z.at[number, z, 0:1]
            send(remote(row, row, sz_send.at[number * 7 + k - 1], sz_recv.at[number * 8 + z], at_z(k)[1]))

    def sums_along_z_end(number):
        for k in range(1, 8):
            w = at_z(k)[0]
            arrived(sum_z.at[number, w, 0:1], sz_recv.at[number * 8 + w])
        sums = sum_z[number, 0, 0:1]
        for k in range(1, 8):
            sums += sum_z[number, k, 0:1]
        w = x * 4 + y
        sum_xy[number, w, 0:1] = sums
        for k in range(1, 16):
            row = sum_xy.at[number, w, 0:1]
            send(remote(row, row, sxy_send.at[number * 15 + k - 1], sxy_recv.at[number * 16 + w], at_xy(k)[1]))

    def scalars(number):
        for k in range(1, 16):
            w = at_xy(k)[0]
            arrived(sum_xy.at[number, w, 0:1], sxy_recv.at[number * 16 + w])
        sums = sum_xy[number, 0, 0:1]
        for k in range(1, 16):
            sums += sum_xy[number, k, 0:1]
        cross_sum, self_sum, diff_sum, mixed_sum, scaled_sum = (
            jnp.sum(jnp.where(lane == k, sums, 0.0), axis=1, keepdims=True) for k in range(5)
        )
        shift = cross_sum / self_sum
        length = diff_sum + 2.0 * shift * mixed_sum + shift * shift * scaled_sum
        shift_out[:, number : number + 1] = shift
        return shift, lax.rsqrt(length / COUNT + 1e-06)

    def whole(pieces):
        return [jnp.concatenate([pieces(k, w) for w in range(4)], axis=0) for k in range(8)]

    def at(k, w):
        return (0, w, k // 2) if k % 2 == 0 else (1, k // 2, w)

    wide = whole(lambda k, w: start_x[at(k, w) + (0,)])
    coupling = coupling_of(jnp.concatenate(wide, axis=1), 0)

    diff, scaled, sums = response_of(trial, coupling)
    along_z(step_z, diff, 1)
    sums_along_z(sums, 0)
    along_z_end(step_z, 1)
    step_x[c, first, second] = jnp.concatenate([step_z[k] for k in range(4)], axis=0).astype(BF16)
    sums_along_z_end(0)
    gather(step_x, 1)
    shift, scale = scalars(0)
    gather_end(step_x, 1)
    trial = (diff + shift * scaled) * scale

    wide = []
    for k in range(8):
        moved = jnp.concatenate([step_x[at(k, w)] for w in range(4)], axis=0).astype(F32)
        old = jnp.concatenate([start_x[at(k, w) + (1,)] for w in range(4)], axis=0).astype(F32)
        wide.append(((moved + shift * old) * scale).astype(BF16))
    coupling = coupling_of(jnp.concatenate(wide, axis=1), 1)

    diff, scaled, sums = response_of(trial, coupling)
    sums_along_z(sums, 1)
    sums_along_z_end(1)
    shift, scale = scalars(1)
    trial = (diff + shift * scaled) * scale
    trial_out[...] = jnp.where(c == 0, trial[:, 0:64], trial[:, 64:128])
    along_z_sent(start_z, 0)
    along_z_sent(step_z, 1)
    for copy in waiting:
        copy.wait_send()


def local(factors, trials, occ_energy, vir_energy):
    vmem, dma = pltpu.VMEM, pltpu.SemaphoreType.DMA
    whole = pl.BlockSpec(memory_space=pltpu.VMEM)
    trial, shifts = pl.pallas_call(
        kernel,
        out_shape=(jax.ShapeDtypeStruct((8, 64), F32), jax.ShapeDtypeStruct((1, 2), F32)),
        in_specs=[pl.BlockSpec(memory_space=pl.ANY), whole, whole, whole],
        out_specs=(whole, whole),
        scratch_shapes=[
            vmem((128, 128), F32),
            vmem((8, 1024, 128), BF16),
            vmem((2, 16, 128), F32),
            vmem((4, 16, 128), BF16),
            vmem((2, 4, 4, 2, 32, 128), BF16),
            vmem((2, 2, 4, 4, 32, 128), BF16),
            vmem((2, 2, 4, 4, 32, 128), BF16),
            vmem((2, 4, 32, 128), BF16),
            vmem((2, 4, 32, 128), BF16),
            vmem((2, 4, 8, 128), F32),
            vmem((2, 8, 8, 128), F32),
            vmem((4, 8, 128), F32),
            vmem((2, 4, 4, 32, 128), BF16),
            vmem((2, 8, 8, 128), F32),
            vmem((2, 16, 8, 128), F32),
            dma((16,)), dma((16,)), dma, dma, dma((14,)), dma((8,)), dma((6,)), dma((8,)), dma((14,)), dma((16,)),
            dma((14,)), dma((16,)), dma((6,)), dma((8,)), dma((16,)), dma((16,)), dma((14,)), dma((16,)), dma((30,)), dma((32,)),
        ],
        compiler_params=pltpu.CompilerParams(collective_id=0, has_side_effects=True),
    )(factors, trials[0].T, occ_energy.reshape(1, 128), vir_energy.reshape(1, 64))
    return trial.T[None], shifts.T


def solution(mesh):
    torus = Mesh(mesh.devices.reshape(4, 4, 4, 2, 2), AUX + VIR_AXES)
    placed = (P(AUX, VIR_AXES, None), P(None, VIR_AXES, AUX), P(), P(VIR_AXES))
    return jax.shard_map(
        local, mesh=torus, in_specs=placed, out_specs=(P(None, VIR_AXES, AUX), P()), check_vma=False
    )
```

```python
import jax
import jax.numpy as jnp
from jax import lax
from jax.experimental import pallas as pl
from jax.experimental.pallas import tpu as pltpu
from jax.sharding import Mesh
from jax.sharding import PartitionSpec as P

AUX = ("aux_0", "aux_1")
VIR_AXES = ("vir_0", "vir_1", "vir_2")
X, ZL, Y, ZH, C = AUX + VIR_AXES
MESH = pl.DeviceIdType.MESH
F32, BF16 = jnp.float32, jnp.bfloat16
COUNT = 1024 * 128


def remote(src, dst, send, recv, device):
    return pltpu.make_async_remote_copy(
        src_ref=src, dst_ref=dst, send_sem=send, recv_sem=recv, device_id=device, device_id_type=MESH
    )


def kernel(
    factors, trials, occ, vir, trial_out, shift_out,
    turn, held, swap, start_z, start_x, first_wide, scaled_wide, part, part_in, tiles, tiles_in,
    step, step_x, sum_z, sum_xy,
    f_send, f_recv, swap_send, swap_recv, az_send, az_recv, as_send, as_recv, af_send, af_recv,
    rf_send, rf_recv, rz_send, rz_recv, step_send, step_recv, sz_send, sz_recv, sxy_send, sxy_recv,
):
    x, zl, y, zh, c = (lax.axis_index(name) for name in (X, ZL, Y, ZH, C))
    z = zh * 4 + zl
    v = y * 4 + zh * 2 + c
    other = 1 - c
    first, second = x + c * (y - x), y + c * (x - y)

    def at_v(k):
        w = lax.rem(v + k, 16)
        return w, {ZL: lax.rem(zl + 2, 4), Y: w // 4, ZH: lax.rem(w // 2, 2), C: lax.rem(w, 2)}

    def at_z(k):
        w = lax.rem(z + k, 8)
        return w, {ZL: lax.rem(w, 4), ZH: w // 4}

    def along(axis, at, k):
        w = lax.rem(at + k, 4)
        return w, {axis: w}

    def at_first(k, core):
        w = lax.rem(first + k, 4)
        return w, {X: x + (1 - c) * (w - x), Y: y + c * (w - y), C: core}

    def at_second(k):
        w = lax.rem(second + k, 4)
        return w, {X: x + c * (w - x), Y: y + (1 - c) * (w - y)}

    def at_xy(k):
        w = lax.rem(x * 4 + y + k, 16)
        return w, {X: w // 4, Y: lax.rem(w, 4)}

    peers = [at_v(k)[1] for k in range(16)] + [at_z(k)[1] for k in range(1, 8)] + [{C: other}]
    for axis, at in ((X, x), (Y, y)):
        for k in range(1, 4):
            peers += [along(axis, at, k)[1] | {C: core} for core in range(2)]
    barrier = pltpu.get_barrier_semaphore()
    for peer in peers:
        pl.semaphore_signal(barrier, inc=1, device_id=peer, device_id_type=MESH)

    mine = lax.broadcasted_iota(jnp.int32, (8, 128), 1) // 64 == c
    swap[0, 0:8] = jnp.where(mine, jnp.concatenate([trials[...], trials[...]], axis=1), 0.0)
    swap[0, 8:16] = jnp.where(mine, jnp.broadcast_to(jnp.concatenate([vir[...], vir[...]], axis=1), (8, 128)), 0.0)
    turn[...] = jnp.transpose(jnp.broadcast_to(occ[...], (128, 128)))
    occ_rows = turn[pl.ds(pl.multiple_of((x * 4 + zl) * 8, 8), 8), :]
    pl.semaphore_wait(barrier, len(peers))

    waiting = []

    def send(copy):
        copy.start()
        waiting.append(copy)

    def drain():
        for copy in waiting:
            copy.wait_send()
        waiting.clear()

    def left(ref, sem):
        remote(ref, ref, sem, swap_recv, {C: other}).wait_send()

    def send_factors(k):
        w, device = at_v(k)
        send(remote(
            factors.at[pl.ds(pl.multiple_of(w * 8, 8), 8)],
            held.at[:, pl.ds(pl.multiple_of(v * 64, 64), 64), :],
            f_send.at[k], f_recv.at[v], device,
        ))

    def arrived(ref, sem):
        remote(ref, ref, swap_send, sem, {C: other}).wait_recv()

    swapped = remote(swap.at[0], swap.at[1], swap_send, swap_recv, {C: other})
    swapped.start()
    for k in range(4):
        send_factors(k)
    swapped.wait()
    full = swap[0] + swap[1]
    trial = full[0:8]
    gap = full[8:16] - occ_rows

    @pl.when(zh == c)
    def _():
        start_z[zl] = jnp.concatenate([trial, trial / gap], axis=0).astype(BF16)
        for k in range(1, 8):
            remote(start_z.at[zl], start_z.at[zl], az_send.at[k - 1], az_recv.at[zl], at_z(k)[1]).start()

    for k in range(4, 16):
        send_factors(k)
    for k in range(1, 4):
        w = lax.rem(zl + k, 4)
        arrived(start_z.at[w], az_recv.at[w])

    @pl.when(zh != c)
    def _():
        arrived(start_z.at[zl], az_recv.at[zl])

    @pl.when(zh == c)
    def _():
        for k in range(1, 8):
            left(start_z.at[zl], az_send.at[k - 1])

    def gather(buffer, number):
        sent, got = number * 7, number * 8
        mine = buffer.at[c, first]
        for k in range(1, 4):
            for core in range(2):
                send(remote(mine, mine, af_send.at[sent + k * 2 - 2 + core], af_recv.at[got + c * 4 + first], at_first(k, core)[1]))
        send(remote(mine, mine, af_send.at[sent + 6], af_recv.at[got + c * 4 + first], {C: other}))

    def gather_end(buffer, number):
        got = number * 8
        for half, at in ((0, x), (1, y)):
            for k in range(1, 4):
                w = lax.rem(at + k, 4)
                arrived(buffer.at[half, w], af_recv.at[got + half * 4 + w])
        far = x + y - first
        arrived(buffer.at[other, far], af_recv.at[got + other * 4 + far])

    for what in range(2):
        pieces = [start_z[k].astype(F32)[what * 8 : what * 8 + 8] for k in range(4)]
        start_x[c, first, second, what] = jnp.concatenate(pieces, axis=0).astype(BF16)
    for k in range(1, 4):
        mine = start_x.at[c, first, second]
        send(remote(mine, mine, as_send.at[k - 1], as_recv.at[second], at_second(k)[1]))
    for k in range(1, 4):
        w = lax.rem(second + k, 4)
        arrived(start_x.at[c, first, w], as_recv.at[w])
    gather(start_x, 0)
    gather_end(start_x, 0)

    def at(k, w):
        return (0, w, k // 2) if k % 2 == 0 else (1, k // 2, w)

    for k in range(8):
        for what, wide in ((0, first_wide), (1, scaled_wide)):
            pieces = [start_x[at(k, w) + (what,)] for w in range(4)]
            wide[:, k * 128 : (k + 1) * 128] = jnp.concatenate(pieces, axis=0)
    for w in range(16):
        arrived(held.at[:, pl.ds(w * 64, 64), :], f_recv.at[w])

    def coupling_of(wide, number):
        eye = (lax.broadcasted_iota(jnp.int32, (128, 128), 0) == lax.broadcasted_iota(jnp.int32, (128, 128), 1)).astype(F32)
        mixed = []
        for q in range(4):
            two = jnp.concatenate([held[2 * q], held[2 * q + 1]], axis=1)
            pairs = jnp.dot(wide, two, preferred_element_type=F32)
            for h in range(2):
                pair = pairs[:, h * 128 : (h + 1) * 128]
                density = jnp.sum(jnp.sum(pair * eye, axis=0, keepdims=True), axis=1, keepdims=True)
                density = density.astype(BF16).astype(F32)
                mixed.append(jnp.transpose(2.0 * density * eye - pair).astype(BF16))
        mixed = jnp.concatenate(mixed, axis=1)
        for q in range(4):
            rows = jnp.concatenate([held[p, q * 256 : (q + 1) * 256, :] for p in range(8)], axis=1)
            block = lax.dot_general(mixed, rows, (((1,), (1,)), ((), ())), preferred_element_type=F32).astype(BF16)
            for w in range(4):
                part[number, 0, w, q] = block[w * 32 : (w + 1) * 32, 0:128]
                part[number, 1, q, w] = block[w * 32 : (w + 1) * 32, 128:256]

        sent, got = number * 7, number * 8
        for half, axis, at in ((0, X, x), (1, Y, y)):
            for k in range(1, 4):
                w, device = along(axis, at, k)
                send(remote(
                    part.at[number, half, w], part_in.at[number, c, at], rf_send.at[sent + half * 3 + k - 1],
                    rf_recv.at[got + c * 4 + at], device | {C: half},
                ))
        far = x + y - first
        send(remote(part.at[number, other, far], part_in.at[number, c, far], rf_send.at[sent + 6], rf_recv.at[got + c * 4 + far], {C: other}))
        total = part[number, c, first].astype(F32)
        arrived(part_in.at[number, other, first], rf_recv.at[got + other * 4 + first])
        total += part_in[number, other, first].astype(F32)
        for k in range(1, 4):
            w = lax.rem(first + k, 4)
            for core in range(2):
                arrived(part_in.at[number, core, w], rf_recv.at[got + core * 4 + w])
                total += part_in[number, core, w].astype(F32)

        for k in range(4):
            for w in range(4):
                tiles[number, k, w] = total[k, w * 8 : (w + 1) * 8].astype(BF16)
        send_sem, recv_sem = rz_send.at[number], rz_recv.at[number]
        slot = tiles_in.at[number, second, z]
        here = zh == c
        for k in range(15, -1, -1):
            s, side = at_second(k // 4)
            w = lax.rem(zl + k % 4, 4)
            for core in range(2):
                if k > 0:
                    remote(tiles.at[number, s, w], slot, send_sem, recv_sem, side | {ZH: c, ZL: w, C: core}).start()
        own = tiles.at[number, second, zl]
        remote(own, slot, send_sem, recv_sem, {ZH: c, C: other}).start()

        @pl.when(here)
        def _():
            pltpu.make_async_copy(own, slot, recv_sem).start()

        @pl.when(jnp.logical_not(here))
        def _():
            remote(own, slot, rz_send.at[2 + number], recv_sem, {ZH: c}).start()

        drain()
        left(tiles.at[number], send_sem)
        left(tiles.at[number, 0:3], send_sem)
        left(tiles.at[number, 3, 0:3], send_sem)

        @pl.when(jnp.logical_not(here))
        def _():
            left(own, rz_send.at[2 + number])

        arrived(tiles_in.at[number], recv_sem)
        coupling = jnp.zeros((8, 128), F32)
        for k in range(4):
            for w in range(8):
                coupling += tiles_in[number, k, w].astype(F32)
        return coupling

    lane = lax.broadcasted_iota(jnp.int32, (1, 128), 1)

    def response_of(trial, coupling):
        response = gap * trial.astype(BF16).astype(F32) + coupling
        diff = trial - response / gap
        scaled = trial / gap
        products = [trial * response, trial * trial, diff * diff, diff * scaled, scaled * scaled]
        sums = jnp.zeros((1, 128), F32)
        for k, product in enumerate(products):
            product = jnp.sum(jnp.sum(product, axis=0, keepdims=True), axis=1, keepdims=True)
            sums = jnp.where(lane == k, product, sums)
        return diff, scaled, sums

    def sums_along_z(sums, number):
        sum_z[number, z, 0:1] = sums
        for k in range(1, 8):
            row = sum_z.at[number, z, 0:1]
            send(remote(row, row, sz_send.at[number * 7 + k - 1], sz_recv.at[number * 8 + z], at_z(k)[1]))

    def sums_along_z_end(number):
        for k in range(1, 8):
            w = at_z(k)[0]
            arrived(sum_z.at[number, w, 0:1], sz_recv.at[number * 8 + w])
        sums = sum_z[number, 0, 0:1]
        for k in range(1, 8):
            sums += sum_z[number, k, 0:1]
        w = x * 4 + y
        sum_xy[number, w, 0:1] = sums
        for k in range(1, 16):
            row = sum_xy.at[number, w, 0:1]
            send(remote(row, row, sxy_send.at[number * 15 + k - 1], sxy_recv.at[number * 16 + w], at_xy(k)[1]))

    def scalars(number):
        for k in range(1, 16):
            w = at_xy(k)[0]
            arrived(sum_xy.at[number, w, 0:1], sxy_recv.at[number * 16 + w])
        sums = sum_xy[number, 0, 0:1]
        for k in range(1, 16):
            sums += sum_xy[number, k, 0:1]
        cross_sum, self_sum, diff_sum, mixed_sum, scaled_sum = (
            jnp.sum(jnp.where(lane == k, sums, 0.0), axis=1, keepdims=True) for k in range(5)
        )
        shift = cross_sum / self_sum
        length = diff_sum + 2.0 * shift * mixed_sum + shift * shift * scaled_sum
        shift_out[:, number : number + 1] = shift
        return shift, lax.rsqrt(length / COUNT + 1e-06)

    coupling = coupling_of(first_wide[...], 0)

    diff, scaled, sums = response_of(trial, coupling)
    step[...] = diff.astype(BF16)
    slot = step_x.at[c, first, second, zl]

    @pl.when(zh == c)
    def _():
        for k in range(31, 0, -1):
            remote(step, slot, step_send, step_recv, at_second(k // 8)[1] | at_z(k % 8)[1]).start()
        pltpu.make_async_copy(step, slot, step_recv).start()

    sums_along_z(sums, 0)
    sums_along_z_end(0)
    arrived(step_x.at[c, first], step_recv)
    gather(step_x, 1)

    @pl.when(zh == c)
    def _():
        left(step_x.at[c, first], step_send)
        left(step_x.at[c, first, 0:3], step_send)
        left(step_x.at[c, first, 3, 0:3], step_send)

    shift, scale = scalars(0)
    gather_end(step_x, 1)
    trial = (diff + shift * scaled) * scale

    wide = []
    for k in range(8):
        moved = [step_x[at(k, w // 4) + (w % 4,)].astype(F32) for w in range(16)]
        moved = jnp.concatenate(moved, axis=0) + shift * scaled_wide[:, k * 128 : (k + 1) * 128].astype(F32)
        wide.append((moved * scale).astype(BF16))
    coupling = coupling_of(jnp.concatenate(wide, axis=1), 1)

    diff, scaled, sums = response_of(trial, coupling)
    sums_along_z(sums, 1)
    sums_along_z_end(1)
    shift, scale = scalars(1)
    trial = (diff + shift * scaled) * scale
    trial_out[...] = jnp.where(c == 0, trial[:, 0:64], trial[:, 64:128])
    drain()


def local(factors, trials, occ_energy, vir_energy):
    vmem, dma = pltpu.VMEM, pltpu.SemaphoreType.DMA
    whole = pl.BlockSpec(memory_space=pltpu.VMEM)
    trial, shifts = pl.pallas_call(
        kernel,
        out_shape=(jax.ShapeDtypeStruct((8, 64), F32), jax.ShapeDtypeStruct((1, 2), F32)),
        in_specs=[pl.BlockSpec(memory_space=pl.ANY), whole, whole, whole],
        out_specs=(whole, whole),
        scratch_shapes=[
            vmem((128, 128), F32),
            vmem((8, 1024, 128), BF16),
            vmem((2, 16, 128), F32),
            vmem((4, 16, 128), BF16),
            vmem((2, 4, 4, 2, 32, 128), BF16),
            vmem((128, 1024), BF16),
            vmem((128, 1024), BF16),
            vmem((2, 2, 4, 4, 32, 128), BF16),
            vmem((2, 2, 4, 4, 32, 128), BF16),
            vmem((2, 4, 4, 8, 128), BF16),
            vmem((2, 4, 8, 8, 128), BF16),
            vmem((8, 128), BF16),
            vmem((2, 4, 4, 4, 8, 128), BF16),
            vmem((2, 8, 8, 128), F32),
            vmem((2, 16, 8, 128), F32),
            dma((16,)), dma((16,)), dma, dma, dma((7,)), dma((4,)), dma((3,)), dma((4,)), dma((14,)), dma((16,)),
            dma((14,)), dma((16,)), dma((4,)), dma((2,)), dma, dma, dma((14,)), dma((16,)), dma((30,)), dma((32,)),
        ],
        compiler_params=pltpu.CompilerParams(collective_id=0, has_side_effects=True),
    )(factors, trials[0].T, occ_energy.reshape(1, 128), vir_energy.reshape(1, 64))
    return trial.T[None], shifts.T


def solution(mesh):
    torus = Mesh(mesh.devices.reshape(4, 4, 4, 2, 2), AUX + VIR_AXES)
    placed = (P(AUX, VIR_AXES, None), P(None, VIR_AXES, AUX), P(), P(VIR_AXES))
    return jax.shard_map(
        local, mesh=torus, in_specs=placed, out_specs=(P(None, VIR_AXES, AUX), P()), check_vma=False
    )
```

```python
import jax
import jax.numpy as jnp
from jax import lax
from jax.experimental import pallas as pl
from jax.experimental.pallas import tpu as pltpu
from jax.sharding import Mesh
from jax.sharding import PartitionSpec as P

AUX = ("aux_0", "aux_1")
VIR_AXES = ("vir_0", "vir_1", "vir_2")
X, ZL, Y, ZH, C = AUX + VIR_AXES
MESH = pl.DeviceIdType.MESH
F32, BF16 = jnp.float32, jnp.bfloat16
COUNT = 1024 * 128


def remote(src, dst, send, recv, device):
    return pltpu.make_async_remote_copy(
        src_ref=src, dst_ref=dst, send_sem=send, recv_sem=recv, device_id=device, device_id_type=MESH
    )


def kernel(
    factors, trials_in, occ_in, vir_in, trial_out, shift_out,
    trials, occ, vir, in_sems, turn, held, swap, start_z, start_x, first_wide, scaled_wide, part, part_in, tiles, tiles_in,
    step, step_x, sum_z, sum_xy, keep, keep_in,
    f_send, f_recv, swap_send, swap_recv, az_send, az_recv, as_send, as_recv, af_send, af_recv,
    rf_send, rf_recv, rz_send, rz_recv, step_send, step_recv, sz_send, sz_recv, sxy_send, sxy_recv,
    last_send, last_recv, hand_send, hand_recv,
):
    x, zl, y, zh, c = (lax.axis_index(name) for name in (X, ZL, Y, ZH, C))
    z = zh * 4 + zl
    v = y * 4 + zh * 2 + c
    other = 1 - c
    first, second = x + c * (y - x), y + c * (x - y)

    def at_v(k):
        w = lax.rem(v + k, 16)
        return w, {ZL: lax.rem(zl + 2, 4), Y: w // 4, ZH: lax.rem(w // 2, 2), C: lax.rem(w, 2)}

    def at_z(k):
        w = lax.rem(z + k, 8)
        return w, {ZL: lax.rem(w, 4), ZH: w // 4}

    def along(axis, at, k):
        w = lax.rem(at + k, 4)
        return w, {axis: w}

    def at_first(k, core):
        w = lax.rem(first + k, 4)
        return w, {X: x + (1 - c) * (w - x), Y: y + c * (w - y), C: core}

    def at_second(k):
        w = lax.rem(second + k, 4)
        return w, {X: x + c * (w - x), Y: y + (1 - c) * (w - y)}

    def at_xy(k):
        w = lax.rem(x * 4 + y + k, 16)
        return w, {X: w // 4, Y: lax.rem(w, 4)}

    peers = [at_v(k)[1] for k in range(16)] + [at_z(k)[1] for k in range(1, 8)] + [{C: other}]
    for axis, at in ((X, x), (Y, y)):
        for k in range(1, 4):
            peers += [along(axis, at, k)[1] | {C: core} for core in range(2)]
    barrier = pltpu.get_barrier_semaphore()
    for peer in peers:
        pl.semaphore_signal(barrier, inc=1, device_id=peer, device_id_type=MESH)

    inputs = [pltpu.make_async_copy(*pair, in_sems.at[k]) for k, pair in enumerate(((trials_in, trials), (occ_in, occ), (vir_in, vir)))]
    for copy in inputs:
        copy.start()
    for copy in inputs:
        copy.wait()
    mine = lax.broadcasted_iota(jnp.int32, (8, 128), 1) // 64 == c
    swap[0, 0:8] = jnp.where(mine, jnp.concatenate([trials[...], trials[...]], axis=1), 0.0)
    swap[0, 8:16] = jnp.where(mine, jnp.broadcast_to(jnp.concatenate([vir[...], vir[...]], axis=1), (8, 128)), 0.0)
    turn[...] = jnp.transpose(jnp.broadcast_to(occ[...], (128, 128)))
    occ_rows = turn[pl.ds(pl.multiple_of((x * 4 + zl) * 8, 8), 8), :]
    pl.semaphore_wait(barrier, len(peers))

    waiting = []

    def send(copy):
        copy.start()
        waiting.append(copy)

    def drain():
        for copy in waiting:
            copy.wait_send()
        waiting.clear()

    def left(ref, sem):
        remote(ref, ref, sem, swap_recv, {C: other}).wait_send()

    def send_factors(k):
        w, device = at_v(k)
        send(remote(
            factors.at[pl.ds(pl.multiple_of(w * 8, 8), 8)],
            held.at[:, pl.ds(pl.multiple_of(v * 64, 64), 64), :],
            f_send.at[k], f_recv.at[v], device,
        ))

    def arrived(ref, sem):
        remote(ref, ref, swap_send, sem, {C: other}).wait_recv()

    swapped = remote(swap.at[0], swap.at[1], swap_send, swap_recv, {C: other})
    swapped.start()
    for k in range(4):
        send_factors(k)
    swapped.wait()
    full = swap[0] + swap[1]
    trial = full[0:8]
    gap = full[8:16] - occ_rows

    @pl.when(zh == c)
    def _():
        start_z[zl] = jnp.concatenate([trial, trial / gap], axis=0).astype(BF16)
        for k in range(1, 8):
            remote(start_z.at[zl], start_z.at[zl], az_send.at[k - 1], az_recv.at[zl], at_z(k)[1]).start()

    for k in range(4, 16):
        send_factors(k)
    for k in range(1, 4):
        w = lax.rem(zl + k, 4)
        arrived(start_z.at[w], az_recv.at[w])

    @pl.when(zh != c)
    def _():
        arrived(start_z.at[zl], az_recv.at[zl])

    @pl.when(zh == c)
    def _():
        for k in range(1, 8):
            left(start_z.at[zl], az_send.at[k - 1])

    def gather(buffer, number):
        sent, got = number * 7, number * 8
        mine = buffer.at[c, first]
        for k in range(1, 4):
            for core in range(2):
                send(remote(mine, mine, af_send.at[sent + k * 2 - 2 + core], af_recv.at[got + c * 4 + first], at_first(k, core)[1]))
        send(remote(mine, mine, af_send.at[sent + 6], af_recv.at[got + c * 4 + first], {C: other}))

    def gather_end(buffer, number):
        got = number * 8
        for half, at in ((0, x), (1, y)):
            for k in range(1, 4):
                w = lax.rem(at + k, 4)
                arrived(buffer.at[half, w], af_recv.at[got + half * 4 + w])
        far = x + y - first
        arrived(buffer.at[other, far], af_recv.at[got + other * 4 + far])

    for what in range(2):
        pieces = [start_z[k].astype(F32)[what * 8 : what * 8 + 8] for k in range(4)]
        start_x[c, first, second, what] = jnp.concatenate(pieces, axis=0).astype(BF16)
    for k in range(1, 4):
        mine = start_x.at[c, first, second]
        send(remote(mine, mine, as_send.at[k - 1], as_recv.at[second], at_second(k)[1]))
    for k in range(1, 4):
        w = lax.rem(second + k, 4)
        arrived(start_x.at[c, first, w], as_recv.at[w])
    gather(start_x, 0)
    gather_end(start_x, 0)

    def at(k, w):
        return (0, w, k // 2) if k % 2 == 0 else (1, k // 2, w)

    for k in range(8):
        for what, wide in ((0, first_wide), (1, scaled_wide)):
            pieces = [start_x[at(k, w) + (what,)] for w in range(4)]
            wide[:, k * 128 : (k + 1) * 128] = jnp.concatenate(pieces, axis=0)
    for w in range(16):
        arrived(held.at[:, pl.ds(w * 64, 64), :], f_recv.at[w])

    def coupling_of(wide, number):
        eye = (lax.broadcasted_iota(jnp.int32, (128, 128), 0) == lax.broadcasted_iota(jnp.int32, (128, 128), 1)).astype(F32)
        mixed = []
        for q in range(4):
            two = jnp.concatenate([held[2 * q], held[2 * q + 1]], axis=1)
            pairs = jnp.dot(wide, two, preferred_element_type=F32)
            for h in range(2):
                pair = pairs[:, h * 128 : (h + 1) * 128]
                density = jnp.sum(jnp.sum(pair * eye, axis=0, keepdims=True), axis=1, keepdims=True)
                density = density.astype(BF16).astype(F32)
                mixed.append(jnp.transpose(2.0 * density * eye - pair).astype(BF16))
        mixed = jnp.concatenate(mixed, axis=1)
        for q in range(4):
            rows = jnp.concatenate([held[p, q * 256 : (q + 1) * 256, :] for p in range(8)], axis=1)
            block = lax.dot_general(mixed, rows, (((1,), (1,)), ((), ())), preferred_element_type=F32).astype(BF16)
            for w in range(4):
                part[number, 0, w, q] = block[w * 32 : (w + 1) * 32, 0:128]
                part[number, 1, q, w] = block[w * 32 : (w + 1) * 32, 128:256]

        sent, got = number * 7, number * 8
        for half, axis, at in ((0, X, x), (1, Y, y)):
            for k in range(1, 4):
                w, device = along(axis, at, k)
                send(remote(
                    part.at[number, half, w], part_in.at[number, c, at], rf_send.at[sent + half * 3 + k - 1],
                    rf_recv.at[got + c * 4 + at], device | {C: half},
                ))
        far = x + y - first
        send(remote(part.at[number, other, far], part_in.at[number, c, far], rf_send.at[sent + 6], rf_recv.at[got + c * 4 + far], {C: other}))
        total = part[number, c, first].astype(F32)
        arrived(part_in.at[number, other, first], rf_recv.at[got + other * 4 + first])
        total += part_in[number, other, first].astype(F32)
        for k in range(1, 4):
            w = lax.rem(first + k, 4)
            for core in range(2):
                arrived(part_in.at[number, core, w], rf_recv.at[got + core * 4 + w])
                total += part_in[number, core, w].astype(F32)

        for k in range(4):
            for w in range(4):
                tiles[number, k, w] = total[k, w * 8 : (w + 1) * 8].astype(BF16)
        send_sem, recv_sem = rz_send.at[number], rz_recv.at[number]
        slot = tiles_in.at[number, second, z]
        for k in range(15, 0, -1):
            s, side = at_second(k // 4)
            w = lax.rem(zl + k % 4, 4)
            remote(tiles.at[number, s, w], slot, send_sem, recv_sem, side | {ZH: c, ZL: w, C: 1}).start()
        own = tiles.at[number, second, zl]
        here = jnp.logical_and(c == 1, zh == 1)

        @pl.when(here)
        def _():
            pltpu.make_async_copy(own, slot, recv_sem).start()

        @pl.when(jnp.logical_not(here))
        def _():
            remote(own, slot, rz_send.at[2 + number], recv_sem, {ZH: c, C: 1}).start()

        drain()
        left(tiles.at[number, 0:3], send_sem)
        left(tiles.at[number, 3, 0:3], send_sem)

        @pl.when(jnp.logical_not(here))
        def _():
            left(own, rz_send.at[2 + number])

    def coupling_sum(number):
        arrived(tiles_in.at[number], rz_recv.at[number])
        coupling = jnp.zeros((8, 128), F32)
        for k in range(4):
            for w in range(8):
                coupling += tiles_in[number, k, w].astype(F32)
        return coupling

    lane = lax.broadcasted_iota(jnp.int32, (1, 128), 1)

    def response_of(trial, coupling):
        response = gap * trial.astype(BF16).astype(F32) + coupling
        diff = trial - response / gap
        scaled = trial / gap
        products = [trial * response, trial * trial, diff * diff, diff * scaled, scaled * scaled]
        sums = jnp.zeros((1, 128), F32)
        for k, product in enumerate(products):
            product = jnp.sum(jnp.sum(product, axis=0, keepdims=True), axis=1, keepdims=True)
            sums = jnp.where(lane == k, product, sums)
        return diff, scaled, sums

    def spread(sums, number):
        sum_z[number, z, 0:1] = sums
        row = sum_z.at[number, z, 0:1]
        copies = [remote(row, row, sz_send.at[number * 7 + k - 1], sz_recv.at[number * 8 + z], at_z(k)[1]) for k in range(1, 8)]
        for copy in copies:
            copy.start()
        for k in range(1, 8):
            w = at_z(k)[0]
            arrived(sum_z.at[number, w, 0:1], sz_recv.at[number * 8 + w])
        sums = sum_z[number, 0, 0:1]
        for k in range(1, 8):
            sums += sum_z[number, k, 0:1]
        w = x * 4 + y
        sum_xy[number, w, 0:1] = sums
        row = sum_xy.at[number, w, 0:1]
        recv_sem = sxy_recv.at[number * 16 + w]
        for core in (1, 0):
            for k in range(core, 16):
                copies.append(remote(row, row, sxy_send.at[number * 31 + core * 15 + k], recv_sem, at_xy(k)[1] | {C: core}))
                copies[-1].start()
        for copy in copies:
            copy.wait_send()

    def scalars(number):
        @pl.when(c == 0)
        def _():
            w = x * 4 + y
            arrived(sum_xy.at[number, w, 0:1], sxy_recv.at[number * 16 + w])

        for k in range(1, 16):
            w = at_xy(k)[0]
            arrived(sum_xy.at[number, w, 0:1], sxy_recv.at[number * 16 + w])
        sums = sum_xy[number, 0, 0:1]
        for k in range(1, 16):
            sums += sum_xy[number, k, 0:1]
        cross_sum, self_sum, diff_sum, mixed_sum, scaled_sum = (
            jnp.sum(jnp.where(lane == k, sums, 0.0), axis=1, keepdims=True) for k in range(5)
        )
        shift = cross_sum / self_sum
        length = diff_sum + 2.0 * shift * mixed_sum + shift * shift * scaled_sum
        shift_out[:, number : number + 1] = shift
        return shift, lax.rsqrt(length / COUNT + 1e-06)

    coupling_of(first_wide[...], 0)

    @pl.when(c == 1)
    def _():
        diff, scaled, sums = response_of(trial, coupling_sum(0))
        keep[0] = diff
        keep[1] = scaled
        step[...] = diff.astype(BF16)
        f, s = x + zh * (y - x), y + zh * (x - y)
        slot = step_x.at[zh, f, s, zl]
        recv_sem = step_recv.at[s]
        for k in range(31, 0, -1):
            w = lax.rem(s + k // 8, 4)
            side = {X: x + zh * (w - x), Y: y + (1 - zh) * (w - y), C: zh}
            remote(step, slot, step_send.at[0], recv_sem, side | at_z(k % 8)[1]).start()

        @pl.when(zh == 1)
        def _():
            pltpu.make_async_copy(step, slot, recv_sem).start()

        @pl.when(zh == 0)
        def _():
            remote(step, slot, step_send.at[1], recv_sem, {C: 0}).start()

        spread(sums, 0)
        left(step_x.at[zh, f], step_send.at[0])
        left(step_x.at[zh, f, 0:3], step_send.at[0])
        left(step_x.at[zh, f, 3, 0:3], step_send.at[0])

        @pl.when(zh == 0)
        def _():
            left(step, step_send.at[1])

    for n, step_at in enumerate((0, 1, 3, 2)):
        w = lax.rem(second + step_at, 4)
        mine = step_x.at[c, first, w]
        arrived(mine, step_recv.at[w])
        recv_sem = last_recv.at[c * 4 + first]
        for k in range(1, 4):
            for core in range(2):
                send(remote(mine, mine, last_send.at[n * 7 + k * 2 - 2 + core], recv_sem, at_first(k, core)[1]))
        send(remote(mine, mine, last_send.at[n * 7 + 6], recv_sem, {C: other}))

    shift, scale = scalars(0)
    for half, side in ((0, x), (1, y)):
        for k in range(1, 4):
            w = lax.rem(side + k, 4)
            arrived(step_x.at[half, w], last_recv.at[half * 4 + w])
    far = x + y - first
    arrived(step_x.at[other, far], last_recv.at[other * 4 + far])

    wide = []
    for k in range(8):
        moved = [step_x[at(k, w // 4) + (w % 4,)].astype(F32) for w in range(16)]
        moved = jnp.concatenate(moved, axis=0) + shift * scaled_wide[:, k * 128 : (k + 1) * 128].astype(F32)
        wide.append((moved * scale).astype(BF16))
    coupling_of(jnp.concatenate(wide, axis=1), 1)

    @pl.when(c == 1)
    def _():
        diff, scaled, sums = response_of((keep[0] + shift * keep[1]) * scale, coupling_sum(1))
        keep[0] = diff
        keep[1] = scaled
        handed = remote(keep, keep_in, hand_send, hand_recv, {C: 0})
        handed.start()
        spread(sums, 1)
        handed.wait_send()

    shift, scale = scalars(1)

    @pl.when(c == 0)
    def _():
        arrived(keep_in, hand_recv)
        trial_out[...] = ((keep_in[0] + shift * keep_in[1]) * scale)[:, 0:64]

    @pl.when(c == 1)
    def _():
        trial_out[...] = ((keep[0] + shift * keep[1]) * scale)[:, 64:128]

    drain()


def local(factors, trials, occ_energy, vir_energy):
    vmem, dma = pltpu.VMEM, pltpu.SemaphoreType.DMA
    whole = pl.BlockSpec(memory_space=pltpu.VMEM)
    trial, shifts = pl.pallas_call(
        kernel,
        out_shape=(pltpu.VMEM((8, 64), F32), pltpu.VMEM((1, 2), F32)),
        in_specs=[pl.BlockSpec(memory_space=pl.ANY)] * 4,
        out_specs=(whole, whole),
        scratch_shapes=[
            vmem((8, 64), F32),
            vmem((1, 128), F32),
            vmem((1, 64), F32),
            dma((3,)),
            vmem((128, 128), F32),
            vmem((8, 1024, 128), BF16),
            vmem((2, 16, 128), F32),
            vmem((4, 16, 128), BF16),
            vmem((2, 4, 4, 2, 32, 128), BF16),
            vmem((128, 1024), BF16),
            vmem((128, 1024), BF16),
            vmem((2, 2, 4, 4, 32, 128), BF16),
            vmem((2, 2, 4, 4, 32, 128), BF16),
            vmem((2, 4, 4, 8, 128), BF16),
            vmem((2, 4, 8, 8, 128), BF16),
            vmem((8, 128), BF16),
            vmem((2, 4, 4, 4, 8, 128), BF16),
            vmem((2, 8, 8, 128), F32),
            vmem((2, 16, 8, 128), F32),
            vmem((2, 8, 128), F32),
            vmem((2, 8, 128), F32),
            dma((16,)), dma((16,)), dma, dma, dma((7,)), dma((4,)), dma((3,)), dma((4,)), dma((14,)), dma((16,)),
            dma((14,)), dma((16,)), dma((4,)), dma((2,)), dma((2,)), dma((4,)), dma((14,)), dma((16,)), dma((62,)), dma((32,)),
            dma((28,)), dma((8,)), dma, dma,
        ],
        compiler_params=pltpu.CompilerParams(collective_id=0, has_side_effects=True),
    )(factors, trials[0].T, occ_energy.reshape(1, 128), vir_energy.reshape(1, 64))
    return trial.T[None], shifts.T


def solution(mesh):
    torus = Mesh(mesh.devices.reshape(4, 4, 4, 2, 2), AUX + VIR_AXES)
    placed = (P(AUX, VIR_AXES, None), P(None, VIR_AXES, AUX), P(), P(VIR_AXES))
    return jax.shard_map(
        local, mesh=torus, in_specs=placed, out_specs=(P(None, VIR_AXES, AUX), P()), check_vma=False
    )
```

```python
import jax
import jax.numpy as jnp
from jax import lax
from jax.experimental import pallas as pl
from jax.experimental.pallas import tpu as pltpu
from jax.sharding import Mesh
from jax.sharding import PartitionSpec as P

AUX = ("aux_0", "aux_1")
VIR_AXES = ("vir_0", "vir_1", "vir_2")
X, ZL, Y, ZH, C = AUX + VIR_AXES
MESH = pl.DeviceIdType.MESH
F32, BF16 = jnp.float32, jnp.bfloat16
COUNT = 1024 * 128


def remote(src, dst, send, recv, device):
    return pltpu.make_async_remote_copy(
        src_ref=src, dst_ref=dst, send_sem=send, recv_sem=recv, device_id=device, device_id_type=MESH
    )


def kernel(
    factors, trials_in, occ_in, vir_in, trial_out, shift_out,
    trials, occ, vir, in_sems, turn, held, swap, start_z, start_x, first_wide, scaled_wide, part, part_in, tiles, tiles_in,
    step, step_x, sum_z, sum_xy, keep, keep_in,
    f_send, f_recv, swap_send, swap_recv, az_send, az_recv, as_send, as_recv, af_send, af_recv,
    rf_send, rf_recv, rz_send, rz_recv, step_send, step_recv, sz_send, sz_recv, sxy_send, sxy_recv,
    last_send, last_recv, hand_send, hand_recv,
):
    x, zl, y, zh, c = (lax.axis_index(name) for name in (X, ZL, Y, ZH, C))
    z = zh * 4 + zl
    v = y * 4 + zh * 2 + c
    other = 1 - c
    first, second = x + c * (y - x), y + c * (x - y)

    def at_v(k):
        w = lax.rem(v + k, 16)
        return w, {ZL: lax.rem(zl + 2, 4), Y: w // 4, ZH: lax.rem(w // 2, 2), C: lax.rem(w, 2)}

    def at_z(k):
        w = lax.rem(z + k, 8)
        return w, {ZL: lax.rem(w, 4), ZH: w // 4}

    def along(axis, at, k):
        w = lax.rem(at + k, 4)
        return w, {axis: w}

    def at_first(k, core):
        w = lax.rem(first + k, 4)
        return w, {X: x + (1 - c) * (w - x), Y: y + c * (w - y), C: core}

    def at_second(k):
        w = lax.rem(second + k, 4)
        return w, {X: x + c * (w - x), Y: y + (1 - c) * (w - y)}

    def at_xy(k):
        w = lax.rem(x * 4 + y + k, 16)
        return w, {X: w // 4, Y: lax.rem(w, 4)}

    peers = [at_v(k)[1] for k in range(16)] + [at_z(k)[1] for k in range(1, 8)] + [{C: other}]
    for axis, at in ((X, x), (Y, y)):
        for k in range(1, 4):
            peers += [along(axis, at, k)[1] | {C: core} for core in range(2)]
    barrier = pltpu.get_barrier_semaphore()
    for peer in peers:
        pl.semaphore_signal(barrier, inc=1, device_id=peer, device_id_type=MESH)

    inputs = [pltpu.make_async_copy(*pair, in_sems.at[k]) for k, pair in enumerate(((trials_in, trials), (occ_in, occ), (vir_in, vir)))]
    for copy in inputs:
        copy.start()
    for copy in inputs:
        copy.wait()
    mine = lax.broadcasted_iota(jnp.int32, (8, 128), 1) // 64 == c
    swap[0, 0:8] = jnp.where(mine, jnp.concatenate([trials[...], trials[...]], axis=1), 0.0)
    swap[0, 8:16] = jnp.where(mine, jnp.broadcast_to(jnp.concatenate([vir[...], vir[...]], axis=1), (8, 128)), 0.0)
    turn[...] = jnp.transpose(jnp.broadcast_to(occ[...], (128, 128)))
    occ_rows = turn[pl.ds(pl.multiple_of((x * 4 + zl) * 8, 8), 8), :]
    pl.semaphore_wait(barrier, len(peers))

    waiting = []

    def send(copy):
        copy.start()
        waiting.append(copy)

    def drain():
        for copy in waiting:
            copy.wait_send()
        waiting.clear()

    def left(ref, sem):
        remote(ref, ref, sem, swap_recv, {C: other}).wait_send()

    def send_factors(k):
        w, device = at_v(k)
        send(remote(
            factors.at[pl.ds(pl.multiple_of(w * 8, 8), 8)],
            held.at[:, pl.ds(pl.multiple_of(v * 64, 64), 64), :],
            f_send.at[k], f_recv.at[v], device,
        ))

    def arrived(ref, sem):
        remote(ref, ref, swap_send, sem, {C: other}).wait_recv()

    swapped = remote(swap.at[0], swap.at[1], swap_send, swap_recv, {C: other})
    swapped.start()
    for k in range(4):
        send_factors(k)
    swapped.wait()
    full = swap[0] + swap[1]
    trial = full[0:8]
    gap = full[8:16] - occ_rows

    @pl.when(zh == c)
    def _():
        start_z[zl] = jnp.concatenate([trial, trial / gap], axis=0).astype(BF16)
        for k in range(1, 8):
            remote(start_z.at[zl], start_z.at[zl], az_send.at[k - 1], az_recv.at[zl], at_z(k)[1]).start()

    for k in range(4, 16):
        send_factors(k)
    for k in range(1, 4):
        w = lax.rem(zl + k, 4)
        arrived(start_z.at[w], az_recv.at[w])

    @pl.when(zh != c)
    def _():
        arrived(start_z.at[zl], az_recv.at[zl])

    @pl.when(zh == c)
    def _():
        for k in range(1, 8):
            left(start_z.at[zl], az_send.at[k - 1])

    def gather(buffer, number):
        sent, got = number * 7, number * 8
        mine = buffer.at[c, first]
        for k in range(1, 4):
            for core in range(2):
                send(remote(mine, mine, af_send.at[sent + k * 2 - 2 + core], af_recv.at[got + c * 4 + first], at_first(k, core)[1]))
        send(remote(mine, mine, af_send.at[sent + 6], af_recv.at[got + c * 4 + first], {C: other}))

    def gather_end(buffer, number):
        got = number * 8
        for half, at in ((0, x), (1, y)):
            for k in range(1, 4):
                w = lax.rem(at + k, 4)
                arrived(buffer.at[half, w], af_recv.at[got + half * 4 + w])
        far = x + y - first
        arrived(buffer.at[other, far], af_recv.at[got + other * 4 + far])

    for what in range(2):
        pieces = [start_z[k].astype(F32)[what * 8 : what * 8 + 8] for k in range(4)]
        start_x[c, first, second, what] = jnp.concatenate(pieces, axis=0).astype(BF16)
    for k in range(1, 4):
        mine = start_x.at[c, first, second]
        send(remote(mine, mine, as_send.at[k - 1], as_recv.at[second], at_second(k)[1]))
    for k in range(1, 4):
        w = lax.rem(second + k, 4)
        arrived(start_x.at[c, first, w], as_recv.at[w])
    gather(start_x, 0)
    gather_end(start_x, 0)

    def at(k, w):
        return (0, w, k // 2) if k % 2 == 0 else (1, k // 2, w)

    for k in range(8):
        for what, wide in ((0, first_wide), (1, scaled_wide)):
            pieces = [start_x[at(k, w) + (what,)] for w in range(4)]
            wide[:, k * 128 : (k + 1) * 128] = jnp.concatenate(pieces, axis=0)
    for w in range(16):
        arrived(held.at[:, pl.ds(w * 64, 64), :], f_recv.at[w])

    def coupling_of(wide, number):
        eye = (lax.broadcasted_iota(jnp.int32, (128, 128), 0) == lax.broadcasted_iota(jnp.int32, (128, 128), 1)).astype(F32)
        mixed = []
        for q in range(4):
            two = jnp.concatenate([held[2 * q], held[2 * q + 1]], axis=1)
            pairs = jnp.dot(wide, two, preferred_element_type=F32)
            for h in range(2):
                pair = pairs[:, h * 128 : (h + 1) * 128]
                density = jnp.sum(jnp.sum(pair * eye, axis=0, keepdims=True), axis=1, keepdims=True)
                density = density.astype(BF16).astype(F32)
                mixed.append(jnp.transpose(2.0 * density * eye - pair).astype(BF16))
        mixed = jnp.concatenate(mixed, axis=1)
        for q in range(4):
            rows = jnp.concatenate([held[p, q * 256 : (q + 1) * 256, :] for p in range(8)], axis=1)
            block = lax.dot_general(mixed, rows, (((1,), (1,)), ((), ())), preferred_element_type=F32).astype(BF16)
            for w in range(4):
                part[number, 0, w, q] = block[w * 32 : (w + 1) * 32, 0:128]
                part[number, 1, q, w] = block[w * 32 : (w + 1) * 32, 128:256]

        for half, axis, at in ((0, X, x), (1, Y, y)):
            sent, recv_sem = number * 8 + half * 4, rf_recv.at[number * 16 + half * 8 + at * 2 + c]
            slot = part_in.at[number, half, at, c]
            for k in range(1, 4):
                w, device = along(axis, at, k)
                send(remote(part.at[number, half, w], slot, rf_send.at[sent + k], recv_sem, device | {C: 1}))

            @pl.when(c == 0)
            def _():
                remote(part.at[number, half, at], slot, rf_send.at[sent], recv_sem, {C: 1}).start()

    def parts_left(number):
        for half, at in ((0, x), (1, y)):
            @pl.when(c == 0)
            def _():
                left(part.at[number, half, at], rf_send.at[number * 8 + half * 4])

    def reduce_halves(number):
        for half, axis, at, side_axis, side_at in ((0, X, x, Y, y), (1, Y, y, X, x)):
            got = number * 16 + half * 8
            total = part[number, half, at].astype(F32)
            arrived(part_in.at[number, half, at, 0], rf_recv.at[got + at * 2])
            total += part_in[number, half, at, 0].astype(F32)
            for k in range(1, 4):
                w = lax.rem(at + k, 4)
                for core in range(2):
                    arrived(part_in.at[number, half, w, core], rf_recv.at[got + w * 2 + core])
                    total += part_in[number, half, w, core].astype(F32)
            for k in range(4):
                for w in range(4):
                    tiles[number, half, k, w] = total[k, w * 8 : (w + 1) * 8].astype(BF16)
            slot = tiles_in.at[number, side_at, z]
            for k in range(15, 0, -1):
                s, side = along(side_axis, side_at, k // 4)
                w = lax.rem(zl + k % 4, 4)
                remote(tiles.at[number, half, s, w], slot, rz_send.at[number * 4 + half], rz_recv.at[number], side | {ZH: half, ZL: w}).start()
            own = tiles.at[number, half, side_at, zl]

            @pl.when(zh == half)
            def _():
                pltpu.make_async_copy(own, slot, rz_recv.at[number]).start()

            @pl.when(zh != half)
            def _():
                remote(own, slot, rz_send.at[number * 4 + 2 + half], rz_recv.at[number], {ZH: half}).start()

    def tiles_left(number):
        for half, at in ((0, y), (1, x)):
            left(tiles.at[number, half, 0:3], rz_send.at[number * 4 + half])
            left(tiles.at[number, half, 3, 0:3], rz_send.at[number * 4 + half])

            @pl.when(zh != half)
            def _():
                left(tiles.at[number, half, at, zl], rz_send.at[number * 4 + 2 + half])

    def coupling_sum(number):
        arrived(tiles_in.at[number], rz_recv.at[number])
        coupling = jnp.zeros((8, 128), F32)
        for k in range(4):
            for w in range(8):
                coupling += tiles_in[number, k, w].astype(F32)
        return coupling

    lane = lax.broadcasted_iota(jnp.int32, (1, 128), 1)

    def response_of(trial, coupling):
        response = gap * trial.astype(BF16).astype(F32) + coupling
        diff = trial - response / gap
        scaled = trial / gap
        products = [trial * response, trial * trial, diff * diff, diff * scaled, scaled * scaled]
        sums = jnp.zeros((1, 128), F32)
        for k, product in enumerate(products):
            product = jnp.sum(jnp.sum(product, axis=0, keepdims=True), axis=1, keepdims=True)
            sums = jnp.where(lane == k, product, sums)
        return diff, scaled, sums

    def spread(sums, number):
        sum_z[number, z, 0:1] = sums
        row = sum_z.at[number, z, 0:1]
        copies = [remote(row, row, sz_send.at[number * 7 + k - 1], sz_recv.at[number * 8 + z], at_z(k)[1]) for k in range(1, 8)]
        for copy in copies:
            copy.start()
        for k in range(1, 8):
            w = at_z(k)[0]
            arrived(sum_z.at[number, w, 0:1], sz_recv.at[number * 8 + w])
        sums = sum_z[number, 0, 0:1]
        for k in range(1, 8):
            sums += sum_z[number, k, 0:1]
        w = x * 4 + y
        sum_xy[number, w, 0:1] = sums
        row = sum_xy.at[number, w, 0:1]
        recv_sem = sxy_recv.at[number * 16 + w]
        for core in (1, 0):
            for k in range(core, 16):
                copies.append(remote(row, row, sxy_send.at[number * 31 + core * 15 + k], recv_sem, at_xy(k)[1] | {C: core}))
                copies[-1].start()
        return copies

    def scalars(number):
        @pl.when(c == 0)
        def _():
            w = x * 4 + y
            arrived(sum_xy.at[number, w, 0:1], sxy_recv.at[number * 16 + w])

        for k in range(1, 16):
            w = at_xy(k)[0]
            arrived(sum_xy.at[number, w, 0:1], sxy_recv.at[number * 16 + w])
        sums = sum_xy[number, 0, 0:1]
        for k in range(1, 16):
            sums += sum_xy[number, k, 0:1]
        cross_sum, self_sum, diff_sum, mixed_sum, scaled_sum = (
            jnp.sum(jnp.where(lane == k, sums, 0.0), axis=1, keepdims=True) for k in range(5)
        )
        shift = cross_sum / self_sum
        length = diff_sum + 2.0 * shift * mixed_sum + shift * shift * scaled_sum
        shift_out[:, number : number + 1] = shift
        return shift, lax.rsqrt(length / COUNT + 1e-06)

    coupling_of(first_wide[...], 0)

    @pl.when(c == 1)
    def _():
        reduce_halves(0)
        tiles_left(0)
        diff, scaled, sums = response_of(trial, coupling_sum(0))
        keep[0] = diff
        keep[1] = scaled
        step[...] = diff.astype(BF16)
        f, s = x + zh * (y - x), y + zh * (x - y)
        slot = step_x.at[zh, f, s, zl]
        recv_sem = step_recv.at[zh]
        for k in range(31, 0, -1):
            w = lax.rem(s + k // 8, 4)
            side = {X: x + zh * (w - x), Y: y + (1 - zh) * (w - y)}
            remote(step, slot, step_send, recv_sem, side | at_z(k % 8)[1]).start()
        pltpu.make_async_copy(step, slot, recv_sem).start()
        pieces = spread(sums, 0)
        for half, axis, at_axis in ((0, X, x), (1, Y, y)):
            mine = step_x.at[half, at_axis]
            arrived(mine, step_recv.at[half])
            recv_sem = last_recv.at[half * 4 + at_axis]
            for k in range(1, 4):
                for core in range(2):
                    device = along(axis, at_axis, k)[1] | {C: core}
                    pieces.append(remote(mine, mine, last_send.at[half * 7 + k * 2 - 2 + core], recv_sem, device))
            pieces.append(remote(mine, mine, last_send.at[half * 7 + 6], recv_sem, {C: 0}))
            for copy in pieces[-7:]:
                copy.start()
        left(step_x.at[zh, f], step_send)
        left(step_x.at[zh, f, 0:3], step_send)
        left(step_x.at[zh, f, 3, 0:3], step_send)
        for copy in pieces:
            copy.wait_send()

    drain()
    parts_left(0)
    shift, scale = scalars(0)
    for half, side in ((0, x), (1, y)):
        for k in range(1, 4):
            w = lax.rem(side + k, 4)
            arrived(step_x.at[half, w], last_recv.at[half * 4 + w])

        @pl.when(c == 0)
        def _():
            arrived(step_x.at[half, side], last_recv.at[half * 4 + side])

    wide = []
    for k in range(8):
        moved = [step_x[at(k, w // 4) + (w % 4,)].astype(F32) for w in range(16)]
        moved = jnp.concatenate(moved, axis=0) + shift * scaled_wide[:, k * 128 : (k + 1) * 128].astype(F32)
        wide.append((moved * scale).astype(BF16))
    coupling_of(jnp.concatenate(wide, axis=1), 1)

    @pl.when(c == 1)
    def _():
        reduce_halves(1)
        tiles_left(1)
        diff, scaled, sums = response_of((keep[0] + shift * keep[1]) * scale, coupling_sum(1))
        keep[0] = diff
        keep[1] = scaled
        handed = remote(keep, keep_in, hand_send, hand_recv, {C: 0})
        handed.start()
        for copy in spread(sums, 1):
            copy.wait_send()
        handed.wait_send()

    drain()
    parts_left(1)
    shift, scale = scalars(1)

    @pl.when(c == 0)
    def _():
        arrived(keep_in, hand_recv)
        trial_out[...] = ((keep_in[0] + shift * keep_in[1]) * scale)[:, 0:64]

    @pl.when(c == 1)
    def _():
        trial_out[...] = ((keep[0] + shift * keep[1]) * scale)[:, 64:128]


def local(factors, trials, occ_energy, vir_energy):
    vmem, dma = pltpu.VMEM, pltpu.SemaphoreType.DMA
    whole = pl.BlockSpec(memory_space=pltpu.VMEM)
    trial, shifts = pl.pallas_call(
        kernel,
        out_shape=(pltpu.VMEM((8, 64), F32), pltpu.VMEM((1, 2), F32)),
        in_specs=[pl.BlockSpec(memory_space=pl.ANY)] * 4,
        out_specs=(whole, whole),
        scratch_shapes=[
            vmem((8, 64), F32),
            vmem((1, 128), F32),
            vmem((1, 64), F32),
            dma((3,)),
            vmem((128, 128), F32),
            vmem((8, 1024, 128), BF16),
            vmem((2, 16, 128), F32),
            vmem((4, 16, 128), BF16),
            vmem((2, 4, 4, 2, 32, 128), BF16),
            vmem((128, 1024), BF16),
            vmem((128, 1024), BF16),
            vmem((2, 2, 4, 4, 32, 128), BF16),
            vmem((2, 2, 4, 2, 4, 32, 128), BF16),
            vmem((2, 2, 4, 4, 8, 128), BF16),
            vmem((2, 4, 8, 8, 128), BF16),
            vmem((8, 128), BF16),
            vmem((2, 4, 4, 4, 8, 128), BF16),
            vmem((2, 8, 8, 128), F32),
            vmem((2, 16, 8, 128), F32),
            vmem((2, 8, 128), F32),
            vmem((2, 8, 128), F32),
            dma((16,)), dma((16,)), dma, dma, dma((7,)), dma((4,)), dma((3,)), dma((4,)), dma((14,)), dma((16,)),
            dma((16,)), dma((32,)), dma((8,)), dma((2,)), dma, dma((2,)), dma((14,)), dma((16,)), dma((62,)), dma((32,)),
            dma((14,)), dma((8,)), dma, dma,
        ],
        compiler_params=pltpu.CompilerParams(collective_id=0, has_side_effects=True),
    )(factors, trials[0].T, occ_energy.reshape(1, 128), vir_energy.reshape(1, 64))
    return trial.T[None], shifts.T


def solution(mesh):
    torus = Mesh(mesh.devices.reshape(4, 4, 4, 2, 2), AUX + VIR_AXES)
    placed = (P(AUX, VIR_AXES, None), P(None, VIR_AXES, AUX), P(), P(VIR_AXES))
    return jax.shard_map(
        local, mesh=torus, in_specs=placed, out_specs=(P(None, VIR_AXES, AUX), P()), check_vma=False
    )
```

```python
import jax
import jax.numpy as jnp
from jax import lax
from jax.experimental import pallas as pl
from jax.experimental.pallas import tpu as pltpu
from jax.sharding import Mesh
from jax.sharding import PartitionSpec as P

AUX = ("aux_0", "aux_1")
VIR_AXES = ("vir_0", "vir_1", "vir_2")
X, ZL, Y, ZH, C = AUX + VIR_AXES
MESH = pl.DeviceIdType.MESH
F32, BF16 = jnp.float32, jnp.bfloat16
COUNT = 1024 * 128


def remote(src, dst, send, recv, device):
    return pltpu.make_async_remote_copy(
        src_ref=src, dst_ref=dst, send_sem=send, recv_sem=recv, device_id=device, device_id_type=MESH
    )


def kernel(
    factors, trials_in, occ_in, vir_in, trial_out, shift_out,
    trials, occ, vir, in_sems, turn, held, swap, start_z, start_x, first_wide, scaled_wide, first_pairs, part, part_in, tiles, tiles_in,
    step, step_x, sum_z, sum_xy, keep, keep_in,
    f_send, f_recv, swap_send, swap_recv, az_send, az_recv, as_send, as_recv, af_send, af_recv,
    rf_send, rf_recv, rz_send, rz_recv, step_send, step_recv, sz_send, sz_recv, sxy_send, sxy_recv,
    last_send, last_recv, hand_send, hand_recv,
):
    x, zl, y, zh, c = (lax.axis_index(name) for name in (X, ZL, Y, ZH, C))
    z = zh * 4 + zl
    v = y * 4 + zh * 2 + c
    other = 1 - c
    first, second = x + c * (y - x), y + c * (x - y)

    def at_v(k):
        w = lax.rem(v + k, 16)
        return w, {ZL: lax.rem(zl + 2, 4), Y: w // 4, ZH: lax.rem(w // 2, 2), C: lax.rem(w, 2)}

    def at_z(k):
        w = lax.rem(z + k, 8)
        return w, {ZL: lax.rem(w, 4), ZH: w // 4}

    def along(axis, at, k):
        w = lax.rem(at + k, 4)
        return w, {axis: w}

    def at_first(k, core):
        w = lax.rem(first + k, 4)
        return w, {X: x + (1 - c) * (w - x), Y: y + c * (w - y), C: core}

    def at_second(k):
        w = lax.rem(second + k, 4)
        return w, {X: x + c * (w - x), Y: y + (1 - c) * (w - y)}

    def at_xy(k):
        w = lax.rem(x * 4 + y + k, 16)
        return w, {X: w // 4, Y: lax.rem(w, 4)}

    peers = [at_v(k)[1] for k in range(16)] + [at_z(k)[1] for k in range(1, 8)] + [{C: other}]
    for axis, at in ((X, x), (Y, y)):
        for k in range(1, 4):
            peers += [along(axis, at, k)[1] | {C: core} for core in range(2)]
    barrier = pltpu.get_barrier_semaphore()
    for peer in peers:
        pl.semaphore_signal(barrier, inc=1, device_id=peer, device_id_type=MESH)

    inputs = [pltpu.make_async_copy(*pair, in_sems.at[k]) for k, pair in enumerate(((trials_in, trials), (occ_in, occ), (vir_in, vir)))]
    for copy in inputs:
        copy.start()
    for copy in inputs:
        copy.wait()
    mine = lax.broadcasted_iota(jnp.int32, (8, 128), 1) // 64 == c
    swap[0, 0:8] = jnp.where(mine, jnp.concatenate([trials[...], trials[...]], axis=1), 0.0)
    swap[0, 8:16] = jnp.where(mine, jnp.broadcast_to(jnp.concatenate([vir[...], vir[...]], axis=1), (8, 128)), 0.0)
    turn[...] = jnp.transpose(jnp.broadcast_to(occ[...], (128, 128)))
    occ_rows = turn[pl.ds(pl.multiple_of((x * 4 + zl) * 8, 8), 8), :]
    pl.semaphore_wait(barrier, len(peers))

    waiting = []

    def send(copy):
        copy.start()
        waiting.append(copy)

    def drain():
        for copy in waiting:
            copy.wait_send()
        waiting.clear()

    def left(ref, sem):
        remote(ref, ref, sem, swap_recv, {C: other}).wait_send()

    def send_factors(k):
        w, device = at_v(k)
        send(remote(
            factors.at[pl.ds(pl.multiple_of(w * 8, 8), 8)],
            held.at[:, pl.ds(pl.multiple_of(v * 64, 64), 64), :],
            f_send.at[k], f_recv.at[v], device,
        ))

    def arrived(ref, sem):
        remote(ref, ref, swap_send, sem, {C: other}).wait_recv()

    swapped = remote(swap.at[0], swap.at[1], swap_send, swap_recv, {C: other})
    swapped.start()
    for k in range(8, 12):
        send_factors(k)
    swapped.wait()
    full = swap[0] + swap[1]
    trial = full[0:8]
    gap = full[8:16] - occ_rows

    @pl.when(zh == c)
    def _():
        start_z[zl] = jnp.concatenate([trial, trial / gap], axis=0).astype(BF16)
        for k in range(1, 8):
            remote(start_z.at[zl], start_z.at[zl], az_send.at[k - 1], az_recv.at[zl], at_z(k)[1]).start()

    for k in (4, 5, 6, 7, 12, 13, 14, 15, 0, 1, 2, 3):
        send_factors(k)
    for k in range(1, 4):
        w = lax.rem(zl + k, 4)
        arrived(start_z.at[w], az_recv.at[w])

    @pl.when(zh != c)
    def _():
        arrived(start_z.at[zl], az_recv.at[zl])

    @pl.when(zh == c)
    def _():
        for k in range(1, 8):
            left(start_z.at[zl], az_send.at[k - 1])

    def gather(buffer, number):
        sent, got = number * 7, number * 8
        mine = buffer.at[c, first]
        for k in range(1, 4):
            for core in range(2):
                send(remote(mine, mine, af_send.at[sent + k * 2 - 2 + core], af_recv.at[got + c * 4 + first], at_first(k, core)[1]))
        send(remote(mine, mine, af_send.at[sent + 6], af_recv.at[got + c * 4 + first], {C: other}))

    def gather_end(buffer, number):
        got = number * 8
        for half, at in ((0, x), (1, y)):
            for k in range(1, 4):
                w = lax.rem(at + k, 4)
                arrived(buffer.at[half, w], af_recv.at[got + half * 4 + w])
        far = x + y - first
        arrived(buffer.at[other, far], af_recv.at[got + other * 4 + far])

    for what in range(2):
        pieces = [start_z[k].astype(F32)[what * 8 : what * 8 + 8] for k in range(4)]
        start_x[c, first, second, what] = jnp.concatenate(pieces, axis=0).astype(BF16)
    for k in range(1, 4):
        mine = start_x.at[c, first, second]
        send(remote(mine, mine, as_send.at[k - 1], as_recv.at[second], at_second(k)[1]))
    for k in range(1, 4):
        w = lax.rem(second + k, 4)
        arrived(start_x.at[c, first, w], as_recv.at[w])
    gather(start_x, 0)
    gather_end(start_x, 0)

    def at(k, w):
        return (0, w, k // 2) if k % 2 == 0 else (1, k // 2, w)

    for k in range(8):
        for what, wide in ((0, first_wide), (1, scaled_wide)):
            pieces = [start_x[at(k, w) + (what,)] for w in range(4)]
            wide[:, k * 128 : (k + 1) * 128] = jnp.concatenate(pieces, axis=0)
    for n, offset in enumerate((2, 3, 1, 0)):
        q = lax.rem(y + offset, 4)
        for w in range(4):
            slot = held.at[:, pl.ds(pl.multiple_of(q * 256 + w * 64, 64), 64), :]
            arrived(slot, f_recv.at[q * 4 + w])
        rows = pl.ds(pl.multiple_of(q * 256, 256), 256)
        some = first_wide[:, rows]
        for t in range(4):
            two = jnp.concatenate([held[2 * t, rows, :], held[2 * t + 1, rows, :]], axis=1)
            value = jnp.dot(some, two, preferred_element_type=F32)
            first_pairs[t] = value if n == 0 else first_pairs[t] + value

    def coupling_of(wide, number):
        eye = (lax.broadcasted_iota(jnp.int32, (128, 128), 0) == lax.broadcasted_iota(jnp.int32, (128, 128), 1)).astype(F32)
        mixed = []
        for q in range(4):
            if number == 0:
                pairs = first_pairs[q]
            else:
                two = jnp.concatenate([held[2 * q], held[2 * q + 1]], axis=1)
                pairs = jnp.dot(wide, two, preferred_element_type=F32)
            for h in range(2):
                pair = pairs[:, h * 128 : (h + 1) * 128]
                density = jnp.sum(jnp.sum(pair * eye, axis=0, keepdims=True), axis=1, keepdims=True)
                density = density.astype(BF16).astype(F32)
                mixed.append(jnp.transpose(2.0 * density * eye - pair).astype(BF16))
        mixed = jnp.concatenate(mixed, axis=1)
        for q in range(4):
            rows = jnp.concatenate([held[p, q * 256 : (q + 1) * 256, :] for p in range(8)], axis=1)
            block = lax.dot_general(mixed, rows, (((1,), (1,)), ((), ())), preferred_element_type=F32).astype(BF16)
            for w in range(4):
                part[number, 0, w, q] = block[w * 32 : (w + 1) * 32, 0:128]
                part[number, 1, q, w] = block[w * 32 : (w + 1) * 32, 128:256]

        for half, axis, at in ((0, X, x), (1, Y, y)):
            sent, recv_sem = number * 8 + half * 4, rf_recv.at[number * 16 + half * 8 + at * 2 + c]
            slot = part_in.at[number, half, at, c]
            for k in range(1, 4):
                w, device = along(axis, at, k)
                send(remote(part.at[number, half, w], slot, rf_send.at[sent + k], recv_sem, device | {C: 1}))

            @pl.when(c == 0)
            def _():
                remote(part.at[number, half, at], slot, rf_send.at[sent], recv_sem, {C: 1}).start()

    def parts_left(number):
        for half, at in ((0, x), (1, y)):
            @pl.when(c == 0)
            def _():
                left(part.at[number, half, at], rf_send.at[number * 8 + half * 4])

    def reduce_halves(number):
        for half, axis, at, side_axis, side_at in ((0, X, x, Y, y), (1, Y, y, X, x)):
            got = number * 16 + half * 8
            total = part[number, half, at].astype(F32)
            arrived(part_in.at[number, half, at, 0], rf_recv.at[got + at * 2])
            total += part_in[number, half, at, 0].astype(F32)
            for k in range(1, 4):
                w = lax.rem(at + k, 4)
                for core in range(2):
                    arrived(part_in.at[number, half, w, core], rf_recv.at[got + w * 2 + core])
                    total += part_in[number, half, w, core].astype(F32)
            for k in range(4):
                for w in range(4):
                    tiles[number, half, k, w] = total[k, w * 8 : (w + 1) * 8].astype(BF16)
            slot = tiles_in.at[number, side_at, z]
            for k in range(15, 0, -1):
                s, side = along(side_axis, side_at, k // 4)
                w = lax.rem(zl + k % 4, 4)
                remote(tiles.at[number, half, s, w], slot, rz_send.at[number * 4 + half], rz_recv.at[number], side | {ZH: half, ZL: w}).start()
            own = tiles.at[number, half, side_at, zl]

            @pl.when(zh == half)
            def _():
                pltpu.make_async_copy(own, slot, rz_recv.at[number]).start()

            @pl.when(zh != half)
            def _():
                remote(own, slot, rz_send.at[number * 4 + 2 + half], rz_recv.at[number], {ZH: half}).start()

    def tiles_left(number):
        for half, at in ((0, y), (1, x)):
            left(tiles.at[number, half, 0:3], rz_send.at[number * 4 + half])
            left(tiles.at[number, half, 3, 0:3], rz_send.at[number * 4 + half])

            @pl.when(zh != half)
            def _():
                left(tiles.at[number, half, at, zl], rz_send.at[number * 4 + 2 + half])

    def coupling_sum(number):
        arrived(tiles_in.at[number], rz_recv.at[number])
        coupling = jnp.zeros((8, 128), F32)
        for k in range(4):
            for w in range(8):
                coupling += tiles_in[number, k, w].astype(F32)
        return coupling

    lane = lax.broadcasted_iota(jnp.int32, (1, 128), 1)

    def response_of(trial, coupling):
        response = gap * trial.astype(BF16).astype(F32) + coupling
        diff = trial - response / gap
        scaled = trial / gap
        products = [trial * response, trial * trial, diff * diff, diff * scaled, scaled * scaled]
        sums = jnp.zeros((1, 128), F32)
        for k, product in enumerate(products):
            product = jnp.sum(jnp.sum(product, axis=0, keepdims=True), axis=1, keepdims=True)
            sums = jnp.where(lane == k, product, sums)
        return diff, scaled, sums

    def spread(sums, number):
        sum_z[number, z, 0:1] = sums
        row = sum_z.at[number, z, 0:1]
        copies = [remote(row, row, sz_send.at[number * 7 + k - 1], sz_recv.at[number * 8 + z], at_z(k)[1]) for k in range(1, 8)]
        for copy in copies:
            copy.start()
        for k in range(1, 8):
            w = at_z(k)[0]
            arrived(sum_z.at[number, w, 0:1], sz_recv.at[number * 8 + w])
        sums = sum_z[number, 0, 0:1]
        for k in range(1, 8):
            sums += sum_z[number, k, 0:1]
        w = x * 4 + y
        sum_xy[number, w, 0:1] = sums
        row = sum_xy.at[number, w, 0:1]
        recv_sem = sxy_recv.at[number * 16 + w]
        for core in (1, 0):
            for k in range(core, 16):
                copies.append(remote(row, row, sxy_send.at[number * 31 + core * 15 + k], recv_sem, at_xy(k)[1] | {C: core}))
                copies[-1].start()
        return copies

    def scalars(number):
        @pl.when(c == 0)
        def _():
            w = x * 4 + y
            arrived(sum_xy.at[number, w, 0:1], sxy_recv.at[number * 16 + w])

        for k in range(1, 16):
            w = at_xy(k)[0]
            arrived(sum_xy.at[number, w, 0:1], sxy_recv.at[number * 16 + w])
        sums = sum_xy[number, 0, 0:1]
        for k in range(1, 16):
            sums += sum_xy[number, k, 0:1]
        cross_sum, self_sum, diff_sum, mixed_sum, scaled_sum = (
            jnp.sum(jnp.where(lane == k, sums, 0.0), axis=1, keepdims=True) for k in range(5)
        )
        shift = cross_sum / self_sum
        length = diff_sum + 2.0 * shift * mixed_sum + shift * shift * scaled_sum
        shift_out[:, number : number + 1] = shift
        return shift, lax.rsqrt(length / COUNT + 1e-06)

    coupling_of(None, 0)

    @pl.when(c == 1)
    def _():
        reduce_halves(0)
        tiles_left(0)
        diff, scaled, sums = response_of(trial, coupling_sum(0))
        keep[0] = diff
        keep[1] = scaled
        step[...] = diff.astype(BF16)
        f, s = x + zh * (y - x), y + zh * (x - y)
        slot = step_x.at[zh, f, s, zl]
        recv_sem = step_recv.at[zh]
        for k in range(31, 0, -1):
            w = lax.rem(s + k // 8, 4)
            side = {X: x + zh * (w - x), Y: y + (1 - zh) * (w - y)}
            remote(step, slot, step_send, recv_sem, side | at_z(k % 8)[1]).start()
        pltpu.make_async_copy(step, slot, recv_sem).start()
        pieces = spread(sums, 0)
        for half, axis, at_axis in ((0, X, x), (1, Y, y)):
            mine = step_x.at[half, at_axis]
            arrived(mine, step_recv.at[half])
            recv_sem = last_recv.at[half * 4 + at_axis]
            for k in range(1, 4):
                for core in range(2):
                    device = along(axis, at_axis, k)[1] | {C: core}
                    pieces.append(remote(mine, mine, last_send.at[half * 7 + k * 2 - 2 + core], recv_sem, device))
            pieces.append(remote(mine, mine, last_send.at[half * 7 + 6], recv_sem, {C: 0}))
            for copy in pieces[-7:]:
                copy.start()
        left(step_x.at[zh, f], step_send)
        left(step_x.at[zh, f, 0:3], step_send)
        left(step_x.at[zh, f, 3, 0:3], step_send)
        for copy in pieces:
            copy.wait_send()

    drain()
    parts_left(0)
    shift, scale = scalars(0)
    for half, side in ((0, x), (1, y)):
        for k in range(1, 4):
            w = lax.rem(side + k, 4)
            arrived(step_x.at[half, w], last_recv.at[half * 4 + w])

        @pl.when(c == 0)
        def _():
            arrived(step_x.at[half, side], last_recv.at[half * 4 + side])

    wide = []
    for k in range(8):
        moved = [step_x[at(k, w // 4) + (w % 4,)].astype(F32) for w in range(16)]
        moved = jnp.concatenate(moved, axis=0) + shift * scaled_wide[:, k * 128 : (k + 1) * 128].astype(F32)
        wide.append((moved * scale).astype(BF16))
    coupling_of(jnp.concatenate(wide, axis=1), 1)

    @pl.when(c == 1)
    def _():
        reduce_halves(1)
        tiles_left(1)
        diff, scaled, sums = response_of((keep[0] + shift * keep[1]) * scale, coupling_sum(1))
        keep[0] = diff
        keep[1] = scaled
        handed = remote(keep, keep_in, hand_send, hand_recv, {C: 0})
        handed.start()
        for copy in spread(sums, 1):
            copy.wait_send()
        handed.wait_send()

    drain()
    parts_left(1)
    shift, scale = scalars(1)

    @pl.when(c == 0)
    def _():
        arrived(keep_in, hand_recv)
        trial_out[...] = ((keep_in[0] + shift * keep_in[1]) * scale)[:, 0:64]

    @pl.when(c == 1)
    def _():
        trial_out[...] = ((keep[0] + shift * keep[1]) * scale)[:, 64:128]


def local(factors, trials, occ_energy, vir_energy):
    vmem, dma = pltpu.VMEM, pltpu.SemaphoreType.DMA
    whole = pl.BlockSpec(memory_space=pltpu.VMEM)
    trial, shifts = pl.pallas_call(
        kernel,
        out_shape=(pltpu.VMEM((8, 64), F32), pltpu.VMEM((1, 2), F32)),
        in_specs=[pl.BlockSpec(memory_space=pl.ANY)] * 4,
        out_specs=(whole, whole),
        scratch_shapes=[
            vmem((8, 64), F32),
            vmem((1, 128), F32),
            vmem((1, 64), F32),
            dma((3,)),
            vmem((128, 128), F32),
            vmem((8, 1024, 128), BF16),
            vmem((2, 16, 128), F32),
            vmem((4, 16, 128), BF16),
            vmem((2, 4, 4, 2, 32, 128), BF16),
            vmem((128, 1024), BF16),
            vmem((128, 1024), BF16),
            vmem((4, 128, 256), F32),
            vmem((2, 2, 4, 4, 32, 128), BF16),
            vmem((2, 2, 4, 2, 4, 32, 128), BF16),
            vmem((2, 2, 4, 4, 8, 128), BF16),
            vmem((2, 4, 8, 8, 128), BF16),
            vmem((8, 128), BF16),
            vmem((2, 4, 4, 4, 8, 128), BF16),
            vmem((2, 8, 8, 128), F32),
            vmem((2, 16, 8, 128), F32),
            vmem((2, 8, 128), F32),
            vmem((2, 8, 128), F32),
            dma((16,)), dma((16,)), dma, dma, dma((7,)), dma((4,)), dma((3,)), dma((4,)), dma((14,)), dma((16,)),
            dma((16,)), dma((32,)), dma((8,)), dma((2,)), dma, dma((2,)), dma((14,)), dma((16,)), dma((62,)), dma((32,)),
            dma((14,)), dma((8,)), dma, dma,
        ],
        compiler_params=pltpu.CompilerParams(collective_id=0, has_side_effects=True),
    )(factors, trials[0].T, occ_energy.reshape(1, 128), vir_energy.reshape(1, 64))
    return trial.T[None], shifts.T


def solution(mesh):
    torus = Mesh(mesh.devices.reshape(4, 4, 4, 2, 2), AUX + VIR_AXES)
    placed = (P(AUX, VIR_AXES, None), P(None, VIR_AXES, AUX), P(), P(VIR_AXES))
    return jax.shard_map(
        local, mesh=torus, in_specs=placed, out_specs=(P(None, VIR_AXES, AUX), P()), check_vma=False
    )
```

```python
import jax
import jax.numpy as jnp
from jax import lax
from jax.experimental import pallas as pl
from jax.experimental.pallas import tpu as pltpu
from jax.sharding import Mesh
from jax.sharding import PartitionSpec as P

AUX = ("aux_0", "aux_1")
VIR_AXES = ("vir_0", "vir_1", "vir_2")
X, ZL, Y, ZH, C = AUX + VIR_AXES
MESH = pl.DeviceIdType.MESH
F32, BF16 = jnp.float32, jnp.bfloat16
COUNT = 1024 * 128


def remote(src, dst, send, recv, device):
    return pltpu.make_async_remote_copy(
        src_ref=src, dst_ref=dst, send_sem=send, recv_sem=recv, device_id=device, device_id_type=MESH
    )


def kernel(
    factors, trials_in, occ_in, vir_in, trial_out, shift_out,
    trials, occ, vir, in_sems, turn, held, swap, start_z, start_x, first_wide, scaled_wide, first_pairs, part, part_in, tiles, tiles_in,
    step, step_x, sum_z, sum_xy, keep, keep_in,
    f_send, f_recv, swap_send, swap_recv, az_send, az_recv, as_send, as_recv, af_send, af_recv,
    rf_send, rf_recv, rz_send, rz_recv, step_send, step_recv, sz_send, sz_recv, sxy_send, sxy_recv,
    last_send, last_recv, hand_send, hand_recv,
):
    x, zl, y, zh, c = (lax.axis_index(name) for name in (X, ZL, Y, ZH, C))
    z = zh * 4 + zl
    v = y * 4 + zh * 2 + c
    other = 1 - c
    first, second = x + c * (y - x), y + c * (x - y)

    def at_v(k):
        w = lax.rem(v + k, 16)
        return w, {ZL: lax.rem(zl + 2, 4), Y: w // 4, ZH: lax.rem(w // 2, 2), C: lax.rem(w, 2)}

    def at_z(k):
        w = lax.rem(z + k, 8)
        return w, {ZL: lax.rem(w, 4), ZH: w // 4}

    def along(axis, at, k):
        w = lax.rem(at + k, 4)
        return w, {axis: w}

    def at_first(k, core):
        w = lax.rem(first + k, 4)
        return w, {X: x + (1 - c) * (w - x), Y: y + c * (w - y), C: core}

    def at_second(k):
        w = lax.rem(second + k, 4)
        return w, {X: x + c * (w - x), Y: y + (1 - c) * (w - y)}

    def at_xy(k):
        w = lax.rem(x * 4 + y + k, 16)
        return w, {X: w // 4, Y: lax.rem(w, 4)}

    inputs = [pltpu.make_async_copy(*pair, in_sems.at[k]) for k, pair in enumerate(((trials_in, trials), (occ_in, occ), (vir_in, vir)))]
    for copy in inputs:
        copy.start()
    peers = [at_v(k)[1] for k in range(16)] + [at_z(k)[1] for k in range(1, 8)] + [{C: other}]
    for axis, at in ((X, x), (Y, y)):
        for k in range(1, 4):
            peers += [along(axis, at, k)[1] | {C: core} for core in range(2)]
    barrier = pltpu.get_barrier_semaphore()
    for peer in peers:
        pl.semaphore_signal(barrier, inc=1, device_id=peer, device_id_type=MESH)

    pl.semaphore_wait(barrier, len(peers))

    waiting = []

    def send(copy):
        copy.start()
        waiting.append(copy)

    def drain():
        for copy in waiting:
            copy.wait_send()
        waiting.clear()

    def left(ref, sem):
        remote(ref, ref, sem, swap_recv, {C: other}).wait_send()

    def send_factors(k):
        w, device = at_v(k)
        send(remote(
            factors.at[pl.ds(pl.multiple_of(w * 8, 8), 8)],
            held.at[:, pl.ds(pl.multiple_of(v * 64, 64), 64), :],
            f_send.at[k], f_recv.at[v], device,
        ))

    def arrived(ref, sem):
        remote(ref, ref, swap_send, sem, {C: other}).wait_recv()

    for k in range(8, 12):
        send_factors(k)
    for copy in inputs:
        copy.wait()
    mine = lax.broadcasted_iota(jnp.int32, (8, 128), 1) // 64 == c
    swap[0, 0:8] = jnp.where(mine, jnp.concatenate([trials[...], trials[...]], axis=1), 0.0)
    swap[0, 8:16] = jnp.where(mine, jnp.broadcast_to(jnp.concatenate([vir[...], vir[...]], axis=1), (8, 128)), 0.0)
    turn[...] = jnp.transpose(jnp.broadcast_to(occ[...], (128, 128)))
    occ_rows = turn[pl.ds(pl.multiple_of((x * 4 + zl) * 8, 8), 8), :]
    swapped = remote(swap.at[0], swap.at[1], swap_send, swap_recv, {C: other})
    swapped.start()
    swapped.wait()
    full = swap[0] + swap[1]
    trial = full[0:8]
    gap = full[8:16] - occ_rows

    @pl.when(zh == c)
    def _():
        start_z[zl] = jnp.concatenate([trial, trial / gap], axis=0).astype(BF16)
        for k in range(1, 8):
            remote(start_z.at[zl], start_z.at[zl], az_send.at[k - 1], az_recv.at[zl], at_z(k)[1]).start()

    for k in (4, 5, 6, 7, 12, 13, 14, 15, 0, 1, 2, 3):
        send_factors(k)
    for k in range(1, 4):
        w = lax.rem(zl + k, 4)
        arrived(start_z.at[w], az_recv.at[w])

    @pl.when(zh != c)
    def _():
        arrived(start_z.at[zl], az_recv.at[zl])

    @pl.when(zh == c)
    def _():
        for k in range(1, 8):
            left(start_z.at[zl], az_send.at[k - 1])

    def gather(buffer, number):
        sent, got = number * 7, number * 8
        mine = buffer.at[c, first]
        for k in range(1, 4):
            for core in range(2):
                send(remote(mine, mine, af_send.at[sent + k * 2 - 2 + core], af_recv.at[got + c * 4 + first], at_first(k, core)[1]))
        send(remote(mine, mine, af_send.at[sent + 6], af_recv.at[got + c * 4 + first], {C: other}))

    def gather_end(buffer, number):
        got = number * 8
        for half, at in ((0, x), (1, y)):
            for k in range(1, 4):
                w = lax.rem(at + k, 4)
                arrived(buffer.at[half, w], af_recv.at[got + half * 4 + w])
        far = x + y - first
        arrived(buffer.at[other, far], af_recv.at[got + other * 4 + far])

    for what in range(2):
        pieces = [start_z[k].astype(F32)[what * 8 : what * 8 + 8] for k in range(4)]
        start_x[c, first, second, what] = jnp.concatenate(pieces, axis=0).astype(BF16)
    for k in range(1, 4):
        mine = start_x.at[c, first, second]
        send(remote(mine, mine, as_send.at[k - 1], as_recv.at[second], at_second(k)[1]))
    for k in range(1, 4):
        w = lax.rem(second + k, 4)
        arrived(start_x.at[c, first, w], as_recv.at[w])
    gather(start_x, 0)
    gather_end(start_x, 0)

    def at(k, w):
        return (0, w, k // 2) if k % 2 == 0 else (1, k // 2, w)

    for k in range(8):
        for what, wide in ((0, first_wide), (1, scaled_wide)):
            pieces = [start_x[at(k, w) + (what,)] for w in range(4)]
            wide[:, k * 128 : (k + 1) * 128] = jnp.concatenate(pieces, axis=0)
    for n, offset in enumerate((2, 3, 1, 0)):
        q = lax.rem(y + offset, 4)
        for w in range(4):
            slot = held.at[:, pl.ds(pl.multiple_of(q * 256 + w * 64, 64), 64), :]
            arrived(slot, f_recv.at[q * 4 + w])
        rows = pl.ds(pl.multiple_of(q * 256, 256), 256)
        some = first_wide[:, rows]
        for t in range(4):
            two = jnp.concatenate([held[2 * t, rows, :], held[2 * t + 1, rows, :]], axis=1)
            value = jnp.dot(some, two, preferred_element_type=F32)
            first_pairs[t] = value if n == 0 else first_pairs[t] + value

    def coupling_of(wide, number):
        eye = (lax.broadcasted_iota(jnp.int32, (128, 128), 0) == lax.broadcasted_iota(jnp.int32, (128, 128), 1)).astype(F32)
        mixed = []
        for q in range(4):
            if number == 0:
                pairs = first_pairs[q]
            else:
                two = jnp.concatenate([held[2 * q], held[2 * q + 1]], axis=1)
                pairs = jnp.dot(wide, two, preferred_element_type=F32)
            for h in range(2):
                pair = pairs[:, h * 128 : (h + 1) * 128]
                density = jnp.sum(jnp.sum(pair * eye, axis=0, keepdims=True), axis=1, keepdims=True)
                density = density.astype(BF16).astype(F32)
                mixed.append(jnp.transpose(2.0 * density * eye - pair).astype(BF16))
        mixed = jnp.concatenate(mixed, axis=1)
        for q in range(4):
            rows = jnp.concatenate([held[p, q * 256 : (q + 1) * 256, :] for p in range(8)], axis=1)
            block = lax.dot_general(mixed, rows, (((1,), (1,)), ((), ())), preferred_element_type=F32).astype(BF16)
            for w in range(4):
                part[number, 0, w, q] = block[w * 32 : (w + 1) * 32, 0:128]
                part[number, 1, q, w] = block[w * 32 : (w + 1) * 32, 128:256]

        for half, axis, at in ((0, X, x), (1, Y, y)):
            sent, recv_sem = number * 8 + half * 4, rf_recv.at[number * 16 + half * 8 + at * 2 + c]
            slot = part_in.at[number, half, at, c]
            for k in range(1, 4):
                w, device = along(axis, at, k)
                send(remote(part.at[number, half, w], slot, rf_send.at[sent + k], recv_sem, device | {C: 1}))

            @pl.when(c == 0)
            def _():
                remote(part.at[number, half, at], slot, rf_send.at[sent], recv_sem, {C: 1}).start()

    def parts_left(number):
        for half, at in ((0, x), (1, y)):
            @pl.when(c == 0)
            def _():
                left(part.at[number, half, at], rf_send.at[number * 8 + half * 4])

    def reduce_halves(number):
        for half, axis, at, side_axis, side_at in ((0, X, x, Y, y), (1, Y, y, X, x)):
            got = number * 16 + half * 8
            total = part[number, half, at].astype(F32)
            arrived(part_in.at[number, half, at, 0], rf_recv.at[got + at * 2])
            total += part_in[number, half, at, 0].astype(F32)
            for k in range(1, 4):
                w = lax.rem(at + k, 4)
                for core in range(2):
                    arrived(part_in.at[number, half, w, core], rf_recv.at[got + w * 2 + core])
                    total += part_in[number, half, w, core].astype(F32)
            for k in range(4):
                for w in range(4):
                    tiles[number, half, k, w] = total[k, w * 8 : (w + 1) * 8].astype(BF16)
            slot = tiles_in.at[number, side_at, z]
            for k in range(15, 0, -1):
                s, side = along(side_axis, side_at, k // 4)
                w = lax.rem(zl + k % 4, 4)
                remote(tiles.at[number, half, s, w], slot, rz_send.at[number * 4 + half], rz_recv.at[number], side | {ZH: half, ZL: w}).start()
            own = tiles.at[number, half, side_at, zl]

            @pl.when(zh == half)
            def _():
                pltpu.make_async_copy(own, slot, rz_recv.at[number]).start()

            @pl.when(zh != half)
            def _():
                remote(own, slot, rz_send.at[number * 4 + 2 + half], rz_recv.at[number], {ZH: half}).start()

    def tiles_left(number):
        for half, at in ((0, y), (1, x)):
            left(tiles.at[number, half, 0:3], rz_send.at[number * 4 + half])
            left(tiles.at[number, half, 3, 0:3], rz_send.at[number * 4 + half])

            @pl.when(zh != half)
            def _():
                left(tiles.at[number, half, at, zl], rz_send.at[number * 4 + 2 + half])

    def coupling_sum(number):
        arrived(tiles_in.at[number], rz_recv.at[number])
        coupling = jnp.zeros((8, 128), F32)
        for k in range(4):
            for w in range(8):
                coupling += tiles_in[number, k, w].astype(F32)
        return coupling

    lane = lax.broadcasted_iota(jnp.int32, (1, 128), 1)

    def response_of(trial, coupling):
        response = gap * trial.astype(BF16).astype(F32) + coupling
        diff = trial - response / gap
        scaled = trial / gap
        products = [trial * response, trial * trial, diff * diff, diff * scaled, scaled * scaled]
        sums = jnp.zeros((1, 128), F32)
        for k, product in enumerate(products):
            product = jnp.sum(jnp.sum(product, axis=0, keepdims=True), axis=1, keepdims=True)
            sums = jnp.where(lane == k, product, sums)
        return diff, scaled, sums

    def spread(sums, number):
        sum_z[number, z, 0:1] = sums
        row = sum_z.at[number, z, 0:1]
        copies = [remote(row, row, sz_send.at[number * 7 + k - 1], sz_recv.at[number * 8 + z], at_z(k)[1]) for k in range(1, 8)]
        for copy in copies:
            copy.start()
        for k in range(1, 8):
            w = at_z(k)[0]
            arrived(sum_z.at[number, w, 0:1], sz_recv.at[number * 8 + w])
        sums = sum_z[number, 0, 0:1]
        for k in range(1, 8):
            sums += sum_z[number, k, 0:1]
        w = x * 4 + y
        sum_xy[number, w, 0:1] = sums
        row = sum_xy.at[number, w, 0:1]
        recv_sem = sxy_recv.at[number * 16 + w]
        for core in (1, 0):
            for k in range(core, 16):
                copies.append(remote(row, row, sxy_send.at[number * 31 + core * 15 + k], recv_sem, at_xy(k)[1] | {C: core}))
                copies[-1].start()
        return copies

    def scalars(number):
        @pl.when(c == 0)
        def _():
            w = x * 4 + y
            arrived(sum_xy.at[number, w, 0:1], sxy_recv.at[number * 16 + w])

        for k in range(1, 16):
            w = at_xy(k)[0]
            arrived(sum_xy.at[number, w, 0:1], sxy_recv.at[number * 16 + w])
        sums = sum_xy[number, 0, 0:1]
        for k in range(1, 16):
            sums += sum_xy[number, k, 0:1]
        cross_sum, self_sum, diff_sum, mixed_sum, scaled_sum = (
            jnp.sum(jnp.where(lane == k, sums, 0.0), axis=1, keepdims=True) for k in range(5)
        )
        shift = cross_sum / self_sum
        length = diff_sum + 2.0 * shift * mixed_sum + shift * shift * scaled_sum
        shift_out[:, number : number + 1] = shift
        return shift, lax.rsqrt(length / COUNT + 1e-06)

    coupling_of(None, 0)

    @pl.when(c == 1)
    def _():
        reduce_halves(0)
        tiles_left(0)
        diff, scaled, sums = response_of(trial, coupling_sum(0))
        keep[0] = diff
        keep[1] = scaled
        step[...] = diff.astype(BF16)
        f, s = x + zh * (y - x), y + zh * (x - y)
        slot = step_x.at[zh, f, s, zl]
        recv_sem = step_recv.at[zh]
        for k in range(31, 0, -1):
            w = lax.rem(s + k // 8, 4)
            side = {X: x + zh * (w - x), Y: y + (1 - zh) * (w - y)}
            remote(step, slot, step_send, recv_sem, side | at_z(k % 8)[1]).start()
        pltpu.make_async_copy(step, slot, recv_sem).start()
        pieces = spread(sums, 0)
        for half, axis, at_axis in ((0, X, x), (1, Y, y)):
            mine = step_x.at[half, at_axis]
            arrived(mine, step_recv.at[half])
            recv_sem = last_recv.at[half * 4 + at_axis]
            for k in range(1, 4):
                for core in range(2):
                    device = along(axis, at_axis, k)[1] | {C: core}
                    pieces.append(remote(mine, mine, last_send.at[half * 7 + k * 2 - 2 + core], recv_sem, device))
            pieces.append(remote(mine, mine, last_send.at[half * 7 + 6], recv_sem, {C: 0}))
            for copy in pieces[-7:]:
                copy.start()
        left(step_x.at[zh, f], step_send)
        left(step_x.at[zh, f, 0:3], step_send)
        left(step_x.at[zh, f, 3, 0:3], step_send)
        for copy in pieces:
            copy.wait_send()

    drain()
    parts_left(0)
    shift, scale = scalars(0)
    for half, side in ((0, x), (1, y)):
        for k in range(1, 4):
            w = lax.rem(side + k, 4)
            arrived(step_x.at[half, w], last_recv.at[half * 4 + w])

        @pl.when(c == 0)
        def _():
            arrived(step_x.at[half, side], last_recv.at[half * 4 + side])

    wide = []
    for k in range(8):
        moved = [step_x[at(k, w // 4) + (w % 4,)].astype(F32) for w in range(16)]
        moved = jnp.concatenate(moved, axis=0) + shift * scaled_wide[:, k * 128 : (k + 1) * 128].astype(F32)
        wide.append((moved * scale).astype(BF16))
    coupling_of(jnp.concatenate(wide, axis=1), 1)

    @pl.when(c == 1)
    def _():
        reduce_halves(1)
        tiles_left(1)
        diff, scaled, sums = response_of((keep[0] + shift * keep[1]) * scale, coupling_sum(1))
        keep[0] = diff
        keep[1] = scaled
        handed = remote(keep, keep_in, hand_send, hand_recv, {C: 0})
        handed.start()
        for copy in spread(sums, 1):
            copy.wait_send()
        handed.wait_send()

    drain()
    parts_left(1)
    shift, scale = scalars(1)

    @pl.when(c == 0)
    def _():
        arrived(keep_in, hand_recv)
        trial_out[...] = ((keep_in[0] + shift * keep_in[1]) * scale)[:, 0:64]

    @pl.when(c == 1)
    def _():
        trial_out[...] = ((keep[0] + shift * keep[1]) * scale)[:, 64:128]


def local(factors, trials, occ_energy, vir_energy):
    vmem, dma = pltpu.VMEM, pltpu.SemaphoreType.DMA
    whole = pl.BlockSpec(memory_space=pltpu.VMEM)
    trial, shifts = pl.pallas_call(
        kernel,
        out_shape=(pltpu.VMEM((8, 64), F32), pltpu.VMEM((1, 2), F32)),
        in_specs=[pl.BlockSpec(memory_space=pl.ANY)] * 4,
        out_specs=(whole, whole),
        scratch_shapes=[
            vmem((8, 64), F32),
            vmem((1, 128), F32),
            vmem((1, 64), F32),
            dma((3,)),
            vmem((128, 128), F32),
            vmem((8, 1024, 128), BF16),
            vmem((2, 16, 128), F32),
            vmem((4, 16, 128), BF16),
            vmem((2, 4, 4, 2, 32, 128), BF16),
            vmem((128, 1024), BF16),
            vmem((128, 1024), BF16),
            vmem((4, 128, 256), F32),
            vmem((2, 2, 4, 4, 32, 128), BF16),
            vmem((2, 2, 4, 2, 4, 32, 128), BF16),
            vmem((2, 2, 4, 4, 8, 128), BF16),
            vmem((2, 4, 8, 8, 128), BF16),
            vmem((8, 128), BF16),
            vmem((2, 4, 4, 4, 8, 128), BF16),
            vmem((2, 8, 8, 128), F32),
            vmem((2, 16, 8, 128), F32),
            vmem((2, 8, 128), F32),
            vmem((2, 8, 128), F32),
            dma((16,)), dma((16,)), dma, dma, dma((7,)), dma((4,)), dma((3,)), dma((4,)), dma((14,)), dma((16,)),
            dma((16,)), dma((32,)), dma((8,)), dma((2,)), dma, dma((2,)), dma((14,)), dma((16,)), dma((62,)), dma((32,)),
            dma((14,)), dma((8,)), dma, dma,
        ],
        compiler_params=pltpu.CompilerParams(collective_id=0, has_side_effects=True),
    )(factors, trials[0].T, occ_energy.reshape(1, 128), vir_energy.reshape(1, 64))
    return trial.T[None], shifts.T


def solution(mesh):
    torus = Mesh(mesh.devices.reshape(4, 4, 4, 2, 2), AUX + VIR_AXES)
    placed = (P(AUX, VIR_AXES, None), P(None, VIR_AXES, AUX), P(), P(VIR_AXES))
    return jax.shard_map(
        local, mesh=torus, in_specs=placed, out_specs=(P(None, VIR_AXES, AUX), P()), check_vma=False
    )
```
